256 devices in a mesh: gx: 16 (over z, core), gy: 16 (over x, y).
Axes of the slice: x: 4, y: 4, z: 8, core: 2. Of those that a mesh axis runs over, the one named last changes fastest.
Arguments:
- tokens: bfloat16 [4096, 4096], P('gx', 'gy'), may hold values from -6 to 6
- gate_blocks: bfloat16 [16, 16, 10, 128, 128], P('gy', 'gx'), may hold values from -0.125 to 0.125
- up_blocks: bfloat16 [16, 16, 10, 128, 128], P('gy', 'gx'), may hold values from -0.125 to 0.125
- gate_coords: int32 [16, 16, 10, 2], P('gy', 'gx'), may hold values from 0 to 6, as said below
- gate_count: int32 [16, 16], P('gy', 'gx'), may hold values from 3 to 10, as said below
- down_blocks: bfloat16 [16, 16, 6, 128, 128], P('gx', 'gy'), may hold values from -0.09375 to 0.09375
- down_rows: int32 [16, 16, 4], P('gx'), may hold values from 0 to 6, as said below
- down_coords: int32 [16, 16, 6, 2], P('gx', 'gy'), may hold values from 0 to 3, as said below
- down_count: int32 [16, 16], P('gx', 'gy'), may hold values from 2 to 6, as said below
Outputs:
- mixed: bfloat16 [4096, 4096], P('gx', 'gy')
The draws below stay inside these ranges and needn't reach their ends.
Inputs may be any that keep to these rules, and one draw needn't show every extreme that they name: `gate_coords`: within each tile the 10 (model-width block, hidden block) pairs are distinct, the first below 2, the second below 7; only the first gate_count slots are live. `gate_count`: some tile has all 10 slots live. `down_rows`: within each down tile the 4 hidden blocks are distinct. `down_coords`: within each down tile the 6 (kept-row index below 4, model-width block below 2) pairs are distinct; only the first down_count slots are live. `down_count`: some tile has all 6 slots live.
All inputs are finite; a program needn't handle non-finite values.
Results may differ from the reference program's by a relative error of at most 0.025.
Values may be sent and summed in bfloat16 or wider, within the bound.
A program may use at most 64 MiB of HBM per device.

```python
import jax
import jax.numpy as jnp
from jax import lax

D = 4096
FF = 14336
BLOCK = 128
TOKENS = 4096
DB = 2
FB = 7
CAP = 10
LOW = 3
USED = 4
CAPD = 6
LOWD = 2
N_GX = 16
N_GY = 16


def tile_pairs(key, tiles, positions, slots, inner):
    tile_keys = jax.random.split(key, tiles)
    orders = jax.vmap(lambda one_key: jax.random.permutation(one_key, positions))(tile_keys)[:, :slots]
    return jnp.stack([orders // inner, orders % inner], -1).astype(jnp.int32)


def tile_counts(key, tiles, lowest, highest):
    counts = jax.random.randint(key, (tiles,), lowest, highest + 1)
    chosen = jax.random.randint(jax.random.fold_in(key, 7), (), 0, tiles)
    return jnp.where(jnp.arange(tiles) == chosen, highest, counts).astype(jnp.int32)


def draw_gate_coords(key, part):
    pairs = tile_pairs(jax.random.fold_in(key, 11), N_GY * N_GX, DB * FB, CAP, FB)
    return pairs.reshape(N_GY, N_GX, CAP, 2)


def draw_gate_count(key, part):
    return tile_counts(jax.random.fold_in(key, 12), N_GY * N_GX, LOW, CAP).reshape(N_GY, N_GX)


def draw_down_rows(key, part):
    tile_keys = jax.random.split(jax.random.fold_in(key, 13), N_GX * N_GY)
    orders = jax.vmap(lambda one_key: jax.random.permutation(one_key, FB))(tile_keys)[:, :USED]
    return orders.astype(jnp.int32).reshape(N_GX, N_GY, USED)


def draw_down_coords(key, part):
    pairs = tile_pairs(jax.random.fold_in(key, 14), N_GX * N_GY, USED * DB, CAPD, DB)
    return pairs.reshape(N_GX, N_GY, CAPD, 2)


def draw_down_count(key, part):
    return tile_counts(jax.random.fold_in(key, 15), N_GX * N_GY, LOWD, CAPD).reshape(N_GX, N_GY)


def shard_levels(rng, shape, cuts, least, high):
    gain, own = 1.0, jax.random.fold_in(rng, 6)
    for dim, shards_of in cuts:
        steps = jnp.exp(jax.random.uniform(jax.random.fold_in(own, dim), (shards_of,), jnp.float32, least / len(cuts), high / len(cuts)))
        gain = gain * jnp.repeat(steps, shape[dim] // shards_of).reshape([-1 if axis == dim else 1 for axis in range(len(shape))])
    return gain


def centred(own_key, extent, scale, limit, cuts=(), held_as=jnp.bfloat16):
    gain = shard_levels(own_key, extent, cuts, -0.22, 0.18) if cuts else 1.0
    values = jax.random.normal(own_key, extent, jnp.float32) * scale * gain
    return jnp.minimum(jnp.maximum(values, -limit), limit).astype(held_as)


def setup_inputs(seed: int = 0) -> dict:
    arg_keys = jax.random.split(jax.random.key(seed), 10)
    tokens = centred(arg_keys[0], (TOKENS, D), 1.0, 6.0, ((0, 16), (1, 16)))
    gate_blocks = centred(arg_keys[1], (N_GY, N_GX, CAP, BLOCK, BLOCK), (D // 2) ** -0.5, 0.125, ((0, 16), (1, 16)))
    up_blocks = centred(arg_keys[2], (N_GY, N_GX, CAP, BLOCK, BLOCK), (D // 2) ** -0.5, 0.125, ((0, 16), (1, 16)))
    gate_coords = draw_gate_coords(jax.random.fold_in(arg_keys[9], 71), 0)
    gate_count = draw_gate_count(jax.random.fold_in(arg_keys[9], 71), 0)
    down_blocks = centred(arg_keys[5], (N_GX, N_GY, CAPD, BLOCK, BLOCK), (FF * 2 // 7) ** -0.5, 0.09375, ((0, 16), (1, 16)))
    down_rows = draw_down_rows(jax.random.fold_in(arg_keys[9], 71), 0)
    down_coords = draw_down_coords(jax.random.fold_in(arg_keys[9], 71), 0)
    down_count = draw_down_count(jax.random.fold_in(arg_keys[9], 71), 0)
    return dict(tokens=tokens, gate_blocks=gate_blocks, up_blocks=up_blocks, gate_coords=gate_coords, gate_count=gate_count, down_blocks=down_blocks, down_rows=down_rows, down_coords=down_coords, down_count=down_count)


def dense_matrix(blocks, local_rows, local_cols, counts, per_row, per_col, row_blocks, col_blocks):
    tiles_a, tiles_b, slots = blocks.shape[0], blocks.shape[1], blocks.shape[2]
    live_slots = jnp.arange(slots, dtype=jnp.int32)[None, None, :] < counts[:, :, None]
    global_rows = jnp.arange(tiles_a, dtype=jnp.int32)[:, None, None] * per_row + local_rows
    global_cols = jnp.arange(tiles_b, dtype=jnp.int32)[None, :, None] * per_col + local_cols
    values = jnp.where(live_slots[..., None, None], blocks, jnp.zeros((), blocks.dtype))
    grid = jnp.zeros((row_blocks, col_blocks, BLOCK, BLOCK), blocks.dtype)
    grid = grid.at[global_rows, global_cols].add(values)
    return grid.transpose(0, 2, 1, 3).reshape(row_blocks * BLOCK, col_blocks * BLOCK)


def rounded_sum(total, term):
    held = lax.optimization_barrier(term.astype(jnp.bfloat16))
    return total + held.astype(jnp.float32)


def reference(tokens, gate_blocks, up_blocks, gate_coords, gate_count, down_blocks, down_rows, down_coords, down_count):
    model_blocks = D // BLOCK
    hidden_blocks = FF // BLOCK
    gate_weight = dense_matrix(gate_blocks, gate_coords[..., 0], gate_coords[..., 1], gate_count, DB, FB, model_blocks, hidden_blocks)
    up_weight = dense_matrix(up_blocks, gate_coords[..., 0], gate_coords[..., 1], gate_count, DB, FB, model_blocks, hidden_blocks)
    kept_rows = jnp.take_along_axis(down_rows, down_coords[..., 0], axis=2)
    down_weight = dense_matrix(down_blocks, kept_rows, down_coords[..., 1], down_count, FB, DB, hidden_blocks, model_blocks)
    gate_total = jnp.zeros((TOKENS, FF), jnp.float32)
    up_total = jnp.zeros((TOKENS, FF), jnp.float32)
    width = DB * BLOCK
    for tile_row in range(N_GY):
        columns = tokens[:, tile_row * width:(tile_row + 1) * width]
        gate_total = rounded_sum(gate_total, jnp.dot(columns, gate_weight[tile_row * width:(tile_row + 1) * width], preferred_element_type=jnp.float32))
        up_total = rounded_sum(up_total, jnp.dot(columns, up_weight[tile_row * width:(tile_row + 1) * width], preferred_element_type=jnp.float32))
    hidden = (jax.nn.silu(gate_total) * up_total).astype(jnp.bfloat16)
    out_total = jnp.zeros((TOKENS, D), jnp.float32)
    span = FB * BLOCK
    for tile_col in range(N_GX):
        part_hidden = hidden[:, tile_col * span:(tile_col + 1) * span]
        out_total = rounded_sum(out_total, jnp.dot(part_hidden, down_weight[tile_col * span:(tile_col + 1) * span], preferred_element_type=jnp.float32))
    return out_total.astype(jnp.bfloat16)
```

```python
import functools

import jax
import jax.numpy as jnp
from jax import lax
from jax.experimental import pallas as pl
from jax.experimental.pallas import tpu as pltpu
from jax.sharding import PartitionSpec as P

MESH = pl.DeviceIdType.MESH
BLOCK = 128
HALF = 64
NX, NY, NZ = 4, 4, 8
DB, FB = 2, 7
CAP, CAPD = 10, 6
TILE = 256
GU = CAP * BLOCK
DOWN_AT = GU
META_AT = GU + CAPD * HALF
PIECE = META_AT + 16
ROWS_A = 160


def place():
    gx, gy = lax.axis_index("gx"), lax.axis_index("gy")
    return lax.div(gy, NY), lax.rem(gy, NY), lax.div(gx, 2), lax.rem(gx, 2)


def dev(x, y, z, c):
    return (2 * z + c, NY * x + y)


def wrap(v, n):
    return lax.rem(v + n, n)


def rcopy(src, dst, send, recv, to):
    return pltpu.make_async_remote_copy(
        src_ref=src, dst_ref=dst, send_sem=send, recv_sem=recv, device_id=to, device_id_type=MESH
    )


def greet(x, y, z, c, partner_self):
    barrier = pltpu.get_barrier_semaphore()

    def hail(to):
        pl.semaphore_signal(barrier, inc=1, device_id=to, device_id_type=MESH)

    hail(dev(wrap(x + 1, NX), y, z, c))
    hail(dev(wrap(x - 1, NX), y, z, c))
    hail(dev(x, y, wrap(z + 1, NZ), c))
    hail(dev(x, y, wrap(z - 1, NZ), c))
    for dy in range(1, NY):
        for flip in range(2):
            hail(dev(x, wrap(y + dy, NY), z, c if flip == 0 else 1 - c))
    hail(dev(x, y, z, 1 - c))

    @pl.when(jnp.logical_not(partner_self))
    def _():
        hail(dev(lax.div(z, 2), y, 2 * x + c, lax.rem(z, 2)))

    pl.semaphore_wait(barrier, 11 + jnp.where(partner_self, 0, 1))


def spread_kernel(packed, tok, wbuf, xbuf, w_send, w_recv, x_send, x_recv):
    x, y, z, c = place()
    t = 1 - 2 * c
    partner_self = z == 2 * x + c
    partner = dev(lax.div(z, 2), y, 2 * x + c, lax.rem(z, 2))
    greet(x, y, z, c, partner_self)
    sent = []
    count = {"w": 0, "x": 0}

    def go(kind, src, dst, to):
        i = count[kind]
        count[kind] += 1
        send, recv = (w_send, w_recv) if kind == "w" else (x_send, x_recv)
        copy = rcopy(src, dst, send.at[i], recv.at[i], to)
        copy.start()
        sent.append(copy)
        return copy

    count["x"] = 1
    mine = xbuf.at[z, y]
    perm = rcopy(tok, xbuf.at[2 * x + c, y], x_send.at[0], x_recv.at[0], partner)

    @pl.when(partner_self)
    def _():
        pltpu.make_async_copy(tok, mine, x_recv.at[0]).start()

    @pl.when(jnp.logical_not(partner_self))
    def _():
        perm.start()

    count["w"] = 2
    firsts = []
    for h in range(2):
        yd, cd = 2 * c + h, lax.rem(y, 2)
        same = jnp.logical_and(yd == y, cd == c)
        slot = lax.div(y, 2)
        copy = rcopy(packed.at[h], wbuf.at[x, y], w_send.at[h], w_recv.at[slot], dev(x, yd, z, cd))

        @pl.when(same)
        def _(h=h, slot=slot):
            pltpu.make_async_copy(packed.at[h], wbuf.at[x, y], w_recv.at[slot]).start()

        @pl.when(jnp.logical_not(same))
        def _(copy=copy):
            copy.start()

        firsts.append((same, copy))

    events = []

    def at(time, fn):
        events.append((time, len(events), fn))

    def piece(dx, q):
        return wbuf.at[wrap(x + dx * t + NX, NX), c + 2 * q]

    sibling = dev(x, y, z, 1 - c)
    fwd, back = dev(wrap(x + t, NX), y, z, c), dev(wrap(x - t, NX), y, z, c)
    handed = []

    def hand(dx, q):
        handed.append(go("w", piece(dx, q), piece(dx, q), sibling))

    for q in range(2):
        ring = {}

        def first(q=q, ring=ring):
            pltpu.make_async_copy(packed.at[0], wbuf.at[x, c + 2 * q], w_recv.at[q]).wait()
            ring["m1"] = go("w", piece(0, q), piece(0, q), fwd)
            ring["o1"] = go("w", piece(0, q), piece(0, q), back)
            hand(0, q)

        def second(q=q, ring=ring):
            ring["m1"].wait_recv()
            ring["m2"] = go("w", piece(-1, q), piece(-1, q), fwd)
            hand(-1, q)

        def third(q=q, ring=ring):
            ring["o1"].wait_recv()
            hand(1, q)

        def fourth(q=q, ring=ring):
            ring["m2"].wait_recv()
            hand(2, q)

        at(7 + q, first)
        at(16 + 6 * q, second)
        at(18 + 6 * q, third)
        at(29 + 6 * q, fourth)

    rows_a, rows_b = pl.ds(0, ROWS_A), pl.ds(ROWS_A, TILE - ROWS_A)
    z_up, z_down = dev(x, y, wrap(z + t, NZ), c), dev(x, y, wrap(z - t, NZ), c)
    y_up, y_down = dev(x, wrap(y + t, NY), z, c), dev(x, wrap(y - t, NY), z, c)
    tails = []

    def block(dz, dy, rows):
        return xbuf.at[wrap(z + dz * t + NZ, NZ), wrap(y + dy * t + NY, NY), rows]

    def spread_y(dz, time, rows):
        ring = {}
        ring["m1"] = go("x", block(dz, 0, rows), block(dz, 0, rows), y_up)
        ring["o1"] = go("x", block(dz, 0, rows), block(dz, 0, rows), y_down)

        def second():
            ring["m1"].wait_recv()
            ring["m2"] = go("x", block(dz, -1, rows), block(dz, -1, rows), y_up)

        def third():
            ring["o1"].wait_recv()
            ring["m2"].wait_recv()

        return second, third

    def bundle(dz):
        return xbuf.at[wrap(z + dz * t + NZ, NZ), :, rows_b]

    state = {"later": []}

    def run_later(time, pair, tail):
        at2.append((time + 4, pair[0]))
        tail.append((time + 8, pair[1]))

    at2 = []

    def start_a():
        pltpu.make_async_copy(tok, mine, x_recv.at[0]).wait()
        state["up"] = go("x", block(0, 0, rows_a), block(0, 0, rows_a), z_up)
        state["down"] = go("x", block(0, 0, rows_a), block(0, 0, rows_a), z_down)
        state["by"] = spread_y(0, 10, rows_b)
        state["ay0"] = spread_y(0, 10, rows_a)

    at(10, start_a)
    for k in range(1, 5):

        def up(k=k):
            state["up"].wait_recv()
            if k < 4:
                state["up"] = go("x", block(-k, 0, rows_a), block(-k, 0, rows_a), z_up)
            state[f"ay{-k}"] = spread_y(-k, 0, rows_a)

        at(10 + 3 * k, up)
        if k < 4:

            def down(k=k):
                state["down"].wait_recv()
                if k < 3:
                    state["down"] = go("x", block(k, 0, rows_a), block(k, 0, rows_a), z_down)
                state[f"ay{k}"] = spread_y(k, 0, rows_a)

            at(10.5 + 3 * k, down)
    for dz in range(-4, 4):
        base = 10 + 3 * abs(dz)
        at(base + 4, lambda dz=dz: state[f"ay{dz}"][0]())
        at(base + 9, lambda dz=dz: state[f"ay{dz}"][1]())
    at(12.5, lambda: state["by"][0]())

    def start_b():
        state["by"][1]()
        state["bup"] = go("x", bundle(0), bundle(0), z_up)
        state["bdown"] = go("x", bundle(0), bundle(0), z_down)

    at(15.5, start_b)
    for k in range(1, 5):

        def bup(k=k):
            state["bup"].wait_recv()
            if k < 4:
                state["bup"] = go("x", bundle(-k), bundle(-k), z_up)

        at(15.5 + 5.5 * k, bup)
        if k < 4:

            def bdown(k=k):
                state["bdown"].wait_recv()
                if k < 3:
                    state["bdown"] = go("x", bundle(k), bundle(k), z_down)

            at(16 + 5.5 * k, bdown)

    for _, _, fn in sorted(events, key=lambda e: e[:2]):
        fn()
    for copy in handed:
        copy.wait_recv()
    for copy in sent:
        copy.wait_send()
    for same, copy in firsts:

        @pl.when(jnp.logical_not(same))
        def _(copy=copy):
            copy.wait_send()

    @pl.when(jnp.logical_not(partner_self))
    def _():
        perm.wait_send()


def spread(packed, tok):
    vmem = pl.BlockSpec(memory_space=pltpu.VMEM)
    return pl.pallas_call(
        spread_kernel,
        out_shape=(
            jax.ShapeDtypeStruct((NX, NY, PIECE, BLOCK), jnp.bfloat16),
            jax.ShapeDtypeStruct((NZ, NY, TILE, TILE), jnp.bfloat16),
        ),
        in_specs=[vmem, vmem],
        out_specs=(vmem, vmem),
        scratch_shapes=[
            pltpu.SemaphoreType.DMA((18,)),
            pltpu.SemaphoreType.DMA((18,)),
            pltpu.SemaphoreType.DMA((48,)),
            pltpu.SemaphoreType.DMA((48,)),
        ],
        compiler_params=pltpu.CompilerParams(
            collective_id=0, has_side_effects=True, vmem_limit_bytes=40 * 2**20
        ),
    )(packed, tok)


def ffn_kernel(meta, wbuf, xbuf, out, dense, acc, hid, dense_d):
    acc[...] = jnp.zeros_like(acc)

    @pl.loop(0, NX * NY)
    def _(a):
        xa, ya = a // NY, a % NY
        for r in range(DB):
            for h in range(FB):
                idx = meta[a, r * FB + h]
                start = pl.multiple_of(jnp.maximum(idx, 0) * BLOCK, BLOCK)
                blk = wbuf[xa, ya, pl.ds(start, BLOCK), :]
                keep = jnp.where(idx >= 0, 1.0, 0.0).astype(jnp.bfloat16)
                dense[r * BLOCK : (r + 1) * BLOCK, h * BLOCK : (h + 1) * BLOCK] = blk * keep
        for s in range(2):
            acc[s * TILE : (s + 1) * TILE, :] += jnp.dot(
                xbuf[2 * xa + s, ya], dense[...], preferred_element_type=jnp.float32
            )

    low = lax.broadcasted_iota(jnp.int32, (2 * TILE, BLOCK), 1) < HALF
    for pair in range(4):
        v = acc[:, 2 * pair * BLOCK : (2 * pair + 1) * BLOCK]
        one = jax.nn.silu(v) * pltpu.roll(v, HALF, 1)
        if 2 * pair + 1 < FB:
            w = acc[:, (2 * pair + 1) * BLOCK : (2 * pair + 2) * BLOCK]
            two = jax.nn.silu(pltpu.roll(w, HALF, 1)) * w
        else:
            two = jnp.zeros_like(one)
        hid[:, pair * BLOCK : (pair + 1) * BLOCK] = jnp.where(low, one, two).astype(jnp.bfloat16)
    dense_d[FB * HALF :, :] = jnp.zeros((HALF, TILE), jnp.bfloat16)

    @pl.loop(0, NX * NY)
    def _(a):
        xa, ya = a // NY, a % NY
        for h in range(FB):
            for m in range(DB):
                idx = meta[a, DB * FB + h * DB + m]
                start = pl.multiple_of(DOWN_AT + jnp.maximum(idx, 0) * HALF, HALF)
                blk = wbuf[xa, ya, pl.ds(start, HALF), :]
                keep = jnp.where(idx >= 0, 1.0, 0.0).astype(jnp.bfloat16)
                dense_d[h * HALF : (h + 1) * HALF, m * BLOCK : (m + 1) * BLOCK] = blk * keep
        for s in range(2):
            out[2 * xa + s, ya] = jnp.dot(
                hid[s * TILE : (s + 1) * TILE, :], dense_d[...], preferred_element_type=jnp.float32
            ).astype(jnp.bfloat16)


def ffn(meta, wbuf, xbuf):
    vmem = pl.BlockSpec(memory_space=pltpu.VMEM)
    return pl.pallas_call(
        ffn_kernel,
        out_shape=jax.ShapeDtypeStruct((NZ, NY, TILE, TILE), jnp.bfloat16),
        in_specs=[pl.BlockSpec(memory_space=pltpu.SMEM), vmem, vmem],
        out_specs=vmem,
        scratch_shapes=[
            pltpu.VMEM((DB * BLOCK, FB * BLOCK), jnp.bfloat16),
            pltpu.VMEM((2 * TILE, FB * BLOCK), jnp.float32),
            pltpu.VMEM((2 * TILE, 4 * BLOCK), jnp.bfloat16),
            pltpu.VMEM((4 * BLOCK, TILE), jnp.bfloat16),
        ],
        compiler_params=pltpu.CompilerParams(vmem_limit_bytes=40 * 2**20),
    )(meta, wbuf, xbuf)


def f32(v):
    return v.astype(jnp.float32)


def gather_kernel(
    part, out,
    ay_in1, ay_in2, ay_in3, ay_out, ay_sum, az_in, az_out,
    bz_in, bz_out, b_sum, by_in, by_out, final, send_sem, recv_sem,
):
    x, y, z, c = place()
    t = 1 - 2 * c
    partner_self = z == 2 * x + c
    partner = dev(lax.div(z, 2), y, 2 * x + c, lax.rem(z, 2))
    greet(x, y, z, c, partner_self)
    rows_a, rows_b = pl.ds(0, ROWS_A), pl.ds(ROWS_A, TILE - ROWS_A)
    z_up, z_down = dev(x, y, wrap(z + t, NZ), c), dev(x, y, wrap(z - t, NZ), c)
    y_up, y_down = dev(x, wrap(y + t, NY), z, c), dev(x, wrap(y - t, NY), z, c)
    sent = []

    def go(src, dst, to):
        i = len(sent)
        copy = rcopy(src, dst, send_sem.at[i], recv_sem.at[i], to)
        copy.start()
        sent.append(copy)
        return copy

    def zz(dz):
        return wrap(z + dz * t + NZ, NZ)

    def yy(dy):
        return wrap(y + dy * t + NY, NY)

    order = [4, -3, 3, -2, 2, -1, 1, 0]
    first, direct, second = {}, {}, {}
    for i, dz in enumerate(order):
        first[i] = go(part.at[zz(dz), yy(2), rows_a], ay_in1.at[i], y_up)
        direct[i] = go(part.at[zz(dz), yy(-1), rows_a], ay_in3.at[i], y_down)
        if i == 0:
            bup = go(part.at[zz(4), :, rows_b], bz_in.at[0], z_up)
            bdown = go(part.at[zz(-3), :, rows_b], bz_in.at[4], z_down)

    up, down = None, None

    def a_first(i):
        first[i].wait_recv()
        ay_out[i] = (f32(ay_in1[i]) + f32(part[zz(order[i]), yy(1), rows_a])).astype(jnp.bfloat16)
        second[i] = go(ay_out.at[i], ay_in2.at[i], y_up)

    def a_sum(i):
        direct[i].wait_recv()
        second[i].wait_recv()
        total = f32(ay_in2[i]) + f32(ay_in3[i]) + f32(part[zz(order[i]), y, rows_a])
        ay_sum[i] = total.astype(jnp.bfloat16)

    def at_dz(dz):
        return order.index(dz)

    def b_up(k, copy):
        copy.wait_recv()
        if k == 4:
            return None
        bz_out[k - 1] = (f32(bz_in[k - 1]) + f32(part[zz(4 - k), :, rows_b])).astype(jnp.bfloat16)
        return go(bz_out.at[k - 1], bz_in.at[k], z_up)

    def b_down(k, copy):
        copy.wait_recv()
        if k == 3:
            return None
        bz_out[k + 2] = (f32(bz_in[k + 3]) + f32(part[zz(k - 3), :, rows_b])).astype(jnp.bfloat16)
        return go(bz_out.at[k + 2], bz_in.at[k + 4], z_down)

    def a_up(k, copy):
        copy.wait_recv()
        if k == 4:
            return None
        az_out[k - 1] = (f32(az_in[k - 1]) + f32(ay_sum[at_dz(4 - k)])).astype(jnp.bfloat16)
        return go(az_out.at[k - 1], az_in.at[k], z_up)

    def a_down(k, copy):
        copy.wait_recv()
        if k == 3:
            return None
        az_out[k + 2] = (f32(az_in[k + 3]) + f32(ay_sum[at_dz(k - 3)])).astype(jnp.bfloat16)
        return go(az_out.at[k + 2], az_in.at[k + 4], z_down)

    a_first(0)
    a_first(1)
    bup = b_up(1, bup)
    bdown = b_down(1, bdown)
    a_first(2)
    a_first(3)
    a_sum(0)
    up = go(ay_sum.at[0], az_in.at[0], z_up)
    a_sum(1)
    down = go(ay_sum.at[1], az_in.at[4], z_down)
    bup = b_up(2, bup)
    bdown = b_down(2, bdown)
    a_first(4)
    a_first(5)
    a_sum(2)
    a_sum(3)
    up = a_up(1, up)
    down = a_down(1, down)
    bup = b_up(3, bup)
    bdown = b_down(3, bdown)
    a_first(6)
    a_first(7)
    a_sum(4)
    a_sum(5)
    up = a_up(2, up)
    down = a_down(2, down)
    b_up(4, bup)
    b_sum[...] = (f32(bz_in[3]) + f32(bz_in[6]) + f32(part[z, :, rows_b])).astype(jnp.bfloat16)
    b1 = go(b_sum.at[yy(2)], by_in.at[0], y_up)
    b3 = go(b_sum.at[yy(-1)], by_in.at[2], y_down)
    a_sum(6)
    a_sum(7)
    up = a_up(3, up)
    b1.wait_recv()
    by_out[...] = (f32(by_in[0]) + f32(b_sum[yy(1)])).astype(jnp.bfloat16)
    b2 = go(by_out, by_in.at[1], y_up)
    b3.wait_recv()
    b2.wait_recv()
    final[rows_b] = (f32(by_in[1]) + f32(by_in[2]) + f32(b_sum[y])).astype(jnp.bfloat16)
    a_down(3, down)
    a_up(4, up)
    final[rows_a] = (f32(az_in[3]) + f32(az_in[6]) + f32(ay_sum[7])).astype(jnp.bfloat16)
    last = rcopy(final, out, send_sem.at[len(sent)], recv_sem.at[len(sent)], partner)

    @pl.when(partner_self)
    def _():
        here = pltpu.make_async_copy(final, out, recv_sem.at[len(sent)])
        here.start()
        here.wait()

    @pl.when(jnp.logical_not(partner_self))
    def _():
        last.start()
        last.wait_recv()
        last.wait_send()

    for copy in sent:
        copy.wait_send()


def collect(part):
    vmem = pl.BlockSpec(memory_space=pltpu.VMEM)
    rb = TILE - ROWS_A
    sems = 24 + 7 + 7 + 3 + 1
    bf = lambda *s: pltpu.VMEM(s, jnp.bfloat16)
    return pl.pallas_call(
        gather_kernel,
        out_shape=jax.ShapeDtypeStruct((TILE, TILE), jnp.bfloat16),
        in_specs=[vmem],
        out_specs=vmem,
        scratch_shapes=[
            bf(8, ROWS_A, TILE), bf(8, ROWS_A, TILE), bf(8, ROWS_A, TILE), bf(8, ROWS_A, TILE), bf(8, ROWS_A, TILE),
            bf(7, ROWS_A, TILE), bf(5, ROWS_A, TILE),
            bf(7, NY, rb, TILE), bf(5, NY, rb, TILE), bf(NY, rb, TILE), bf(3, rb, TILE), bf(rb, TILE),
            bf(TILE, TILE),
            pltpu.SemaphoreType.DMA((sems,)),
            pltpu.SemaphoreType.DMA((sems,)),
        ],
        compiler_params=pltpu.CompilerParams(
            collective_id=1, has_side_effects=True, vmem_limit_bytes=40 * 2**20
        ),
    )(part)


def where_slot(rows, cols, count, per_col, n):
    slots = jnp.arange(rows.shape[0])
    hit = (rows * per_col + cols)[None, :] == jnp.arange(n)[:, None]
    hit = jnp.logical_and(hit, (slots < count)[None, :])
    return jnp.sum(jnp.where(hit, slots[None, :] + 1, 0), axis=1) - 1


def body(
    tokens, gate_blocks, up_blocks, gate_coords, gate_count,
    down_blocks, down_rows, down_coords, down_count,
):
    gate = gate_blocks[0, 0].reshape(GU, 2, HALF)
    up = up_blocks[0, 0].reshape(GU, 2, HALF)
    both = jnp.concatenate([gate, up], -1).transpose(1, 0, 2)
    down = down_blocks[0, 0].reshape(CAPD, 2, HALF, BLOCK).transpose(1, 0, 2, 3).reshape(2, CAPD * HALF, BLOCK)
    g_at = where_slot(gate_coords[0, 0, :, 0], gate_coords[0, 0, :, 1], gate_count[0, 0], FB, DB * FB)
    rows = lax.dynamic_index_in_dim(down_rows[0], lax.axis_index("gy"), 0, False)
    kept = jnp.sum(jnp.where(down_coords[0, 0, :, :1] == jnp.arange(rows.shape[0])[None, :], rows[None, :], 0), 1)
    d_at = where_slot(kept, down_coords[0, 0, :, 1], down_count[0, 0], DB, DB * FB)
    row = jnp.concatenate([g_at, d_at, jnp.zeros((BLOCK - 28,), jnp.int32)]).astype(jnp.bfloat16)
    meta = jnp.broadcast_to(row, (2, 16, BLOCK))
    packed = jnp.concatenate([both, down, meta], 1)
    wbuf, xbuf = spread(packed, tokens)
    table = wbuf[:, :, META_AT, :32].astype(jnp.int32).reshape(NX * NY, 32)
    return collect(ffn(table, wbuf, xbuf))


def solution(mesh):
    return jax.shard_map(
        body,
        mesh=mesh,
        in_specs=(
            P("gx", "gy"),
            P("gy", "gx", None, None, None),
            P("gy", "gx", None, None, None),
            P("gy", "gx", None, None),
            P("gy", "gx"),
            P("gx", "gy", None, None, None),
            P("gx", None, None),
            P("gx", "gy", None, None),
            P("gx", "gy"),
        ),
        out_specs=P("gx", "gy"),
        check_vma=False,
    )
```

```python
import jax
import jax.numpy as jnp
from jax import lax
from jax.experimental import pallas as pl
from jax.experimental.pallas import tpu as pltpu
from jax.sharding import PartitionSpec as P

MESH = pl.DeviceIdType.MESH
BLOCK = 128
HALF = 64
NX, NY, NZ = 4, 4, 8
DB, FB = 2, 7
CAP, CAPD = 10, 6
TILE = 256
GU = CAP * BLOCK
DOWN_AT = GU
META_AT = GU + CAPD * HALF
PIECE = META_AT + 16
WIDE = NY * TILE
HID = FB * HALF
ROWS_A = 160


def place():
    gx, gy = lax.axis_index("gx"), lax.axis_index("gy")
    return lax.div(gy, NY), lax.rem(gy, NY), lax.div(gx, 2), lax.rem(gx, 2)


def dev(x, y, z, c):
    return (2 * z + c, NY * x + y)


def wrap(v, n):
    return lax.rem(v + n, n)


def rcopy(src, dst, send, recv, to):
    return pltpu.make_async_remote_copy(
        src_ref=src, dst_ref=dst, send_sem=send, recv_sem=recv, device_id=to, device_id_type=MESH
    )


def hails(x, y, z, c, partner, partner_self):
    barrier = pltpu.get_barrier_semaphore()

    def hail(to):
        pl.semaphore_signal(barrier, inc=1, device_id=to, device_id_type=MESH)

    hail(dev(wrap(x + 1, NX), y, z, c))
    hail(dev(wrap(x - 1, NX), y, z, c))
    hail(dev(x, y, wrap(z + 1, NZ), c))
    hail(dev(x, y, wrap(z - 1, NZ), c))
    for dy in range(1, NY):
        for flip in range(2):
            hail(dev(x, wrap(y + dy, NY), z, c if flip == 0 else 1 - c))
    hail(dev(x, y, z, 1 - c))

    @pl.when(jnp.logical_not(partner_self))
    def _():
        hail(partner)

    return lambda: pl.semaphore_wait(barrier, 11 + jnp.where(partner_self, 0, 1))


def f32(v):
    return v.astype(jnp.float32)


def bf16(v):
    return v.astype(jnp.bfloat16)


E_AT = {0: 0, -1: 1, 1: 2, 2: 3}
ORDER = [4, -3, 3, -2, 2, -1, 1, 0]


def kernel(
    g_coords, g_count, d_rows, d_coords, d_count,
    tok, gate, up, down, out,
    packed, w_own, w_sib, xb, dgu, dd, acc, hid, part,
    ay_in1, ay_in2, ay_in3, ay_out, ay_sum, az_in, az_out,
    bz_in, bz_out, b_sum, by_in, by_out, final, send_sem, recv_sem,
):
    x, y, z, c = place()
    t = 1 - 2 * c
    partner = dev(lax.div(z, 2), y, 2 * x + c, lax.rem(z, 2))
    partner_self = z == 2 * x + c
    remote_partner = jnp.logical_not(partner_self)
    wait_all_here = hails(x, y, z, c, partner, partner_self)
    sibling = dev(x, y, z, 1 - c)
    x_up, x_down = dev(wrap(x + t, NX), y, z, c), dev(wrap(x - t, NX), y, z, c)
    y_up, y_down = dev(x, wrap(y + t, NY), z, c), dev(x, wrap(y - t, NY), z, c)
    z_up, z_down = dev(x, y, wrap(z + t, NZ), c), dev(x, y, wrap(z - t, NZ), c)
    sent, events, used = [], [], [0]

    def sem():
        used[0] += 1
        return used[0] - 1

    def go(src, dst, to):
        i = sem()
        copy = rcopy(src, dst, send_sem.at[i], recv_sem.at[i], to)
        copy.start()
        sent.append(copy)
        return copy

    def at(time, fn):
        events.append((time, len(events), fn))

    def run():
        for _, _, fn in sorted(events, key=lambda e: e[:2]):
            fn()
        events.clear()

    def xx(dx):
        return wrap(x + dx * t + NX, NX)

    def yy(dy):
        return wrap(y + dy * t + NY, NY)

    def zz(dz):
        return wrap(z + dz * t + NZ, NZ)

    def xblock(zi, yi, row, rows):
        start = pl.multiple_of(lax.rem(zi, 2) * TILE + row, 32)
        return xb.at[lax.div(zi, 2), pl.ds(start, rows), pl.ds(pl.multiple_of(yi * TILE, TILE), TILE)]

    low = lax.broadcasted_iota(jnp.int32, (BLOCK, BLOCK), 1) < HALF
    for s in range(CAP):
        g, u = f32(gate[s]), f32(up[s])
        packed[0, s * BLOCK : (s + 1) * BLOCK, :] = bf16(jnp.where(low, g, pltpu.roll(u, HALF, 1)))
        packed[1, s * BLOCK : (s + 1) * BLOCK, :] = bf16(jnp.where(low, pltpu.roll(g, HALF, 1), u))
    for s in range(CAPD):
        for h in range(2):
            packed[h, DOWN_AT + s * HALF : DOWN_AT + (s + 1) * HALF, :] = down[s, h * HALF : (h + 1) * HALF, :]
    slot_row = lax.broadcasted_iota(jnp.int32, (16, BLOCK), 0)
    ids = jnp.full((16, BLOCK), 99, jnp.int32)
    for s in range(CAP):
        spot = jnp.where(s < g_count[0], g_coords[2 * s] * FB + g_coords[2 * s + 1], 99)
        ids = jnp.where(slot_row == s, spot, ids)
    for s in range(CAPD):
        kept = d_rows[(NY * x + y) * 4 + d_coords[2 * s]]
        spot = jnp.where(s < d_count[0], kept * DB + d_coords[2 * s + 1], 99)
        ids = jnp.where(slot_row == CAP + s, spot, ids)
    for h in range(2):
        packed[h, META_AT:PIECE, :] = bf16(f32(ids))

    wait_all_here()

    perm_at = sem()
    mine = xblock(z, y, 0, TILE)
    perm = rcopy(tok, xblock(2 * x + c, y, 0, TILE), send_sem.at[perm_at], recv_sem.at[perm_at], partner)

    @pl.when(partner_self)
    def _():
        pltpu.make_async_copy(tok, mine, recv_sem.at[perm_at]).start()

    @pl.when(remote_partner)
    def _():
        perm.start()

    w1 = [sem(), sem()]
    firsts = []
    slot, land = lax.rem(y, 2), lax.div(y, 2)
    for h in range(2):
        yd = 2 * c + h
        same = jnp.logical_and(yd == y, land == c)
        dst = w_own.at[0, slot]
        copy = rcopy(packed.at[h], dst, send_sem.at[w1[h]], recv_sem.at[w1[0] + slot], dev(x, yd, z, land))

        @pl.when(same)
        def _(h=h, dst=dst):
            pltpu.make_async_copy(packed.at[h], dst, recv_sem.at[w1[0] + slot]).start()

        @pl.when(jnp.logical_not(same))
        def _(copy=copy):
            copy.start()

        firsts.append((same, copy))

    near = lax.rem(y + jnp.where(land == c, 0, 1), 2)
    handed = {}

    def hand(dx, n, q):
        e = -dx if abs(dx) == 1 else dx
        handed[e, n] = go(w_own.at[E_AT[dx], q], w_sib.at[E_AT[e], q], sibling)

    def build(ref, e, ya0):
        @pl.loop(0, 2)
        def _(q):
            ya = ya0 + q
            xa = xx(e)
            names = f32(ref[E_AT[e], q, META_AT:PIECE, :])
            for r in range(DB):
                for h in range(FB):
                    w = jnp.zeros((BLOCK, BLOCK), jnp.bfloat16)
                    for s in range(CAP):
                        hit = names[s : s + 1, :] == float(r * FB + h)
                        w = jnp.where(hit, ref[E_AT[e], q, s * BLOCK : (s + 1) * BLOCK, :], w)
                    row = pl.multiple_of(ya * TILE + r * BLOCK, BLOCK)
                    dgu[xa, pl.ds(row, BLOCK), h * BLOCK : (h + 1) * BLOCK] = w
            for h in range(FB):
                for m in range(DB):
                    w = jnp.zeros((HALF, BLOCK), jnp.bfloat16)
                    for s in range(CAPD):
                        hit = names[CAP + s : CAP + s + 1, :] == float(h * DB + m)
                        at_row = DOWN_AT + s * HALF
                        w = jnp.where(hit, ref[E_AT[e], q, at_row : at_row + HALF, :], w)
                    dd[xa, ya, h * HALF : (h + 1) * HALF, m * BLOCK : (m + 1) * BLOCK] = w

    def build_own(e):
        build(w_own, e, 2 * c)

    def build_sib(e):
        handed[e, 0].wait_recv()
        handed[e, 1].wait_recv()
        build(w_sib, e, 2 * (1 - c))

    for n in range(2):
        q = near if n == 0 else 1 - near
        ring = {}

        def first(n=n, q=q, ring=ring):
            pltpu.make_async_copy(packed.at[0], w_own.at[0, q], recv_sem.at[w1[0] + q]).wait()
            ring["m1"] = go(w_own.at[0, q], w_own.at[1, q], x_up)
            ring["o1"] = go(w_own.at[0, q], w_own.at[2, q], x_down)
            hand(0, n, q)

        def second(n=n, q=q, ring=ring):
            ring["m1"].wait_recv()
            ring["m2"] = go(w_own.at[1, q], w_own.at[3, q], x_up)
            hand(-1, n, q)

        def third(n=n, q=q, ring=ring):
            ring["o1"].wait_recv()
            hand(1, n, q)

        def fourth(n=n, q=q, ring=ring):
            ring["m2"].wait_recv()
            hand(2, n, q)

        at(5 + 7 * n, first)
        at(12 + 8 * n, second)
        at(13 + 8 * n, third)
        at(21 + 8 * n, fourth)
    at(12.1, lambda: build_own(0))
    at(15.1, lambda: build_sib(0))
    at(21.1, lambda: build_own(-1))
    at(21.2, lambda: build_own(1))
    at(24.1, lambda: build_sib(-1))
    at(24.2, lambda: build_sib(1))

    a_part, b_part = (0, ROWS_A), (ROWS_A, TILE - ROWS_A)

    def pass_on(dz, dy, part_rows, to):
        ref = xblock(zz(dz), yy(dy), *part_rows)
        return go(ref, ref, to)

    def along_y(dz, part_rows, time, then=None):
        ring = {}
        ring["m1"] = pass_on(dz, 0, part_rows, y_up)
        ring["o1"] = pass_on(dz, 0, part_rows, y_down)

        def second():
            ring["m1"].wait_recv()
            ring["m2"] = pass_on(dz, -1, part_rows, y_up)
            if then:
                then(-1)

        def third():
            ring["o1"].wait_recv()
            if then:
                then(1)

        def fourth():
            ring["m2"].wait_recv()
            if then:
                then(2)

        return second, third, fourth

    state = {}

    def z_start(dy):
        state["up", dy] = pass_on(0, dy, b_part, z_up)
        state["down", dy] = pass_on(0, dy, b_part, z_down)

    def z_up_step(k, dy):
        state["up", dy].wait_recv()
        if k < 4:
            state["up", dy] = pass_on(-k, dy, b_part, z_up)

    def z_down_step(k, dy):
        state["down", dy].wait_recv()
        if k < 3:
            state["down", dy] = pass_on(k, dy, b_part, z_down)

    def start_tokens():
        pltpu.make_async_copy(tok, mine, recv_sem.at[perm_at]).wait()
        state["up"] = pass_on(0, 0, a_part, z_up)
        state["down"] = pass_on(0, 0, a_part, z_down)
        state["by"] = along_y(0, b_part, 0, z_start)
        z_start(0)
        state["ay", 0] = along_y(0, a_part, 0)

    at(8, start_tokens)
    for k in range(1, 5):

        def a_up(k=k):
            state["up"].wait_recv()
            if k < 4:
                state["up"] = pass_on(-k, 0, a_part, z_up)
            state["ay", -k] = along_y(-k, a_part, 0)

        def a_down(k=k):
            state["down"].wait_recv()
            if k < 3:
                state["down"] = pass_on(k, 0, a_part, z_down)
            state["ay", k] = along_y(k, a_part, 0)

        at(8 + 3 * k, a_up)
        if k < 4:
            at(8.5 + 3 * k, a_down)
    for dz in range(-4, 4):
        base = 8 + 3 * abs(dz)
        at(base + 3.5, lambda dz=dz: state["ay", dz][0]())
        at(base + 4.0, lambda dz=dz: state["ay", dz][1]())
        at(base + 8.5, lambda dz=dz: state["ay", dz][2]())
    at(11, lambda: state["by"][0]())
    at(11.2, lambda: state["by"][1]())
    at(14, lambda: state["by"][2]())
    for dy, begin in ((0, 8), (-1, 11), (1, 11.3), (2, 14)):
        for k in range(1, 5):
            at(begin + 3.3 * k, lambda k=k, dy=dy: z_up_step(k, dy))
            if k < 4:
                at(begin + 0.3 + 3.3 * k, lambda k=k, dy=dy: z_down_step(k, dy))

    def clear():
        acc[...] = jnp.zeros_like(acc)

        @pl.loop(0, NX * NY)
        def _(a):
            dd[lax.div(a, NY), lax.rem(a, NY), HID:, :] = jnp.zeros((2 * TILE - HID, TILE), jnp.bfloat16)

    at(0, clear)

    def multiply(e):
        for s in range(2):
            acc[s * TILE : (s + 1) * TILE, :] += jnp.dot(
                xb[xx(e), s * TILE : (s + 1) * TILE, :], dgu[xx(e)], preferred_element_type=jnp.float32
            )

    at(40, lambda: multiply(0))
    at(41, lambda: multiply(-1))
    at(42, lambda: multiply(1))
    at(43, lambda: build_own(2))
    at(44, lambda: build_sib(2))
    at(45, lambda: multiply(2))
    run()

    wide = lax.broadcasted_iota(jnp.int32, (2 * TILE, BLOCK), 1) < HALF
    for pair in range(4):
        v = acc[:, 2 * pair * BLOCK : (2 * pair + 1) * BLOCK]
        one = jax.nn.silu(v) * pltpu.roll(v, HALF, 1)
        if 2 * pair + 1 < FB:
            w = acc[:, (2 * pair + 1) * BLOCK : (2 * pair + 2) * BLOCK]
            two = jax.nn.silu(pltpu.roll(w, HALF, 1)) * w
        else:
            two = jnp.zeros_like(one)
        hid[:, pair * BLOCK : (pair + 1) * BLOCK] = bf16(jnp.where(wide, one, two))

    rows_a, rows_b = pl.ds(0, ROWS_A), pl.ds(ROWS_A, TILE - ROWS_A)
    DYS = (2, -1, 1, 0)
    first, direct, second = {}, {}, {}

    def project(i):
        dz = ORDER[i]
        zi = zz(dz)
        mine_rows = hid[pl.ds(pl.multiple_of(lax.rem(zi, 2) * TILE, TILE), TILE), :]
        for j, dy in enumerate(DYS):
            part[zi, yy(dy)] = bf16(
                jnp.dot(mine_rows, dd[lax.div(zi, 2), yy(dy)], preferred_element_type=jnp.float32)
            )
            if dy == 2:
                first[i] = go(part.at[zi, yy(2), rows_a], ay_in1.at[i], y_up)
            if dy == -1:
                direct[i] = go(part.at[zi, yy(-1), rows_a], ay_in3.at[i], y_down)
            if dz == 4:
                state["bu", j] = go(part.at[zi, yy(dy), rows_b], bz_in.at[0, j], z_up)
            if dz == -3:
                state["bd", j] = go(part.at[zi, yy(dy), rows_b], bz_in.at[4, j], z_down)

    def a_first(i):
        first[i].wait_recv()
        ay_out[i] = bf16(f32(ay_in1[i]) + f32(part[zz(ORDER[i]), yy(1), rows_a]))
        second[i] = go(ay_out.at[i], ay_in2.at[i], y_up)

    def a_sum(i):
        direct[i].wait_recv()
        second[i].wait_recv()
        ay_sum[i] = bf16(f32(ay_in2[i]) + f32(ay_in3[i]) + f32(part[zz(ORDER[i]), y, rows_a]))
        if ORDER[i] == 4:
            state["au"] = go(ay_sum.at[i], az_in.at[0], z_up)
        if ORDER[i] == -3:
            state["ad"] = go(ay_sum.at[i], az_in.at[4], z_down)

    def chain_a_up(k):
        state["au"].wait_recv()
        if k < 4:
            az_out[k - 1] = bf16(f32(az_in[k - 1]) + f32(ay_sum[ORDER.index(4 - k)]))
            state["au"] = go(az_out.at[k - 1], az_in.at[k], z_up)

    def chain_a_down(k):
        state["ad"].wait_recv()
        if k < 3:
            az_out[k + 2] = bf16(f32(az_in[k + 3]) + f32(ay_sum[ORDER.index(k - 3)]))
            state["ad"] = go(az_out.at[k + 2], az_in.at[k + 4], z_down)

    def chain_b_up(k, j):
        state["bu", j].wait_recv()
        if k < 4:
            bz_out[k - 1, j] = bf16(f32(bz_in[k - 1, j]) + f32(part[zz(4 - k), yy(DYS[j]), rows_b]))
            state["bu", j] = go(bz_out.at[k - 1, j], bz_in.at[k, j], z_up)

    def chain_b_down(k, j):
        state["bd", j].wait_recv()
        if k < 3:
            bz_out[k + 2, j] = bf16(f32(bz_in[k + 3, j]) + f32(part[zz(k - 3), yy(DYS[j]), rows_b]))
            state["bd", j] = go(bz_out.at[k + 2, j], bz_in.at[k + 4, j], z_down)

    def b_end(j):
        b_sum[j] = bf16(f32(bz_in[3, j]) + f32(bz_in[6, j]) + f32(part[z, yy(DYS[j]), rows_b]))
        if j == 0:
            state["by1"] = go(b_sum.at[0], by_in.at[0], y_up)
        if j == 1:
            state["by3"] = go(b_sum.at[1], by_in.at[2], y_down)

    def b_relay():
        state["by1"].wait_recv()
        by_out[...] = bf16(f32(by_in[0]) + f32(b_sum[2]))
        state["by2"] = go(by_out, by_in.at[1], y_up)

    lasts = []

    def deliver(rows):
        i = sem()
        copy = rcopy(final.at[rows], out.at[rows], send_sem.at[i], recv_sem.at[i], partner)
        here = pltpu.make_async_copy(final.at[rows], out.at[rows], recv_sem.at[i])

        @pl.when(partner_self)
        def _():
            here.start()

        @pl.when(remote_partner)
        def _():
            copy.start()

        lasts.append((copy, here))

    def b_last():
        state["by3"].wait_recv()
        state["by2"].wait_recv()
        final[rows_b] = bf16(f32(by_in[1]) + f32(by_in[2]) + f32(b_sum[3]))
        deliver(rows_b)

    def a_last():
        final[rows_a] = bf16(f32(az_in[3]) + f32(az_in[6]) + f32(ay_sum[7]))
        deliver(rows_a)

    for i in range(8):
        at(0.8 * i, lambda i=i: project(i))
        at(3.2 + 2.6 * i, lambda i=i: a_first(i))
        at(6.5 + 2.6 * i, lambda i=i: a_sum(i))
    for j in range(4):
        for k in range(1, 5):
            at(3.5 + 0.7 * j + 5 * (k - 1), lambda k=k, j=j: chain_b_up(k, j))
            if k < 4:
                at(4.5 + 0.7 * j + 5 * (k - 1), lambda k=k, j=j: chain_b_down(k, j))
        at(3.6 + 0.7 * j + 15, lambda j=j: b_end(j))
    at(23, b_relay)
    at(27, b_last)
    for k in range(1, 5):
        at(11.8 + 5.2 * (k - 1), lambda k=k: chain_a_up(k))
        if k < 4:
            at(14.4 + 5.2 * (k - 1), lambda k=k: chain_a_down(k))
    at(28, a_last)
    run()

    for copy in sent:
        copy.wait_send()
    for same, copy in firsts:

        @pl.when(jnp.logical_not(same))
        def _(copy=copy):
            copy.wait_send()

    @pl.when(remote_partner)
    def _():
        perm.wait_send()

    for copy, here in lasts:
        here.wait()

        @pl.when(remote_partner)
        def _(copy=copy):
            copy.wait_send()


SEMS = 170


def body(
    tokens, gate_blocks, up_blocks, gate_coords, gate_count,
    down_blocks, down_rows, down_coords, down_count,
):
    vmem, smem = pl.BlockSpec(memory_space=pltpu.VMEM), pl.BlockSpec(memory_space=pltpu.SMEM)
    rb = TILE - ROWS_A
    bf = lambda *s: pltpu.VMEM(s, jnp.bfloat16)
    return pl.pallas_call(
        kernel,
        out_shape=jax.ShapeDtypeStruct((TILE, TILE), jnp.bfloat16),
        in_specs=[smem] * 5 + [vmem] * 4,
        out_specs=vmem,
        scratch_shapes=[
            bf(2, PIECE, BLOCK), bf(4, 2, PIECE, BLOCK), bf(4, 2, PIECE, BLOCK),
            bf(NX, 2 * TILE, WIDE), bf(NX, WIDE, FB * BLOCK), bf(NX, NY, 2 * TILE, TILE),
            pltpu.VMEM((2 * TILE, FB * BLOCK), jnp.float32), bf(2 * TILE, 2 * TILE),
            bf(NZ, NY, TILE, TILE),
            bf(8, ROWS_A, TILE), bf(8, ROWS_A, TILE), bf(8, ROWS_A, TILE), bf(8, ROWS_A, TILE), bf(8, ROWS_A, TILE),
            bf(7, ROWS_A, TILE), bf(5, ROWS_A, TILE),
            bf(7, NY, rb, TILE), bf(5, NY, rb, TILE), bf(NY, rb, TILE), bf(3, rb, TILE), bf(rb, TILE),
            bf(TILE, TILE),
            pltpu.SemaphoreType.DMA((SEMS,)),
            pltpu.SemaphoreType.DMA((SEMS,)),
        ],
        compiler_params=pltpu.CompilerParams(
            collective_id=0, has_side_effects=True, vmem_limit_bytes=58 * 2**20
        ),
    )(
        gate_coords.reshape(-1), gate_count.reshape(-1), down_rows.reshape(-1),
        down_coords.reshape(-1), down_count.reshape(-1),
        tokens, gate_blocks[0, 0], up_blocks[0, 0], down_blocks[0, 0],
    )


def solution(mesh):
    return jax.shard_map(
        body,
        mesh=mesh,
        in_specs=(
            P("gx", "gy"),
            P("gy", "gx", None, None, None),
            P("gy", "gx", None, None, None),
            P("gy", "gx", None, None),
            P("gy", "gx"),
            P("gx", "gy", None, None, None),
            P("gx", None, None),
            P("gx", "gy", None, None),
            P("gx", "gy"),
        ),
        out_specs=P("gx", "gy"),
        check_vma=False,
    )
```

```python
import jax
import jax.numpy as jnp
from jax import lax
from jax.experimental import pallas as pl
from jax.experimental.pallas import tpu as pltpu
from jax.sharding import PartitionSpec as P

MESH = pl.DeviceIdType.MESH
BLOCK = 128
HALF = 64
NX, NY, NZ = 4, 4, 8
DB, FB = 2, 7
CAP, CAPD = 10, 6
TILE = 256
GU = CAP * BLOCK
DOWN_AT = GU
META_AT = GU + CAPD * HALF
PIECE = META_AT + 32
PART = PIECE // 2
WIDE = NY * TILE
HID = FB * HALF
ROWS_A = 160


def place():
    gx, gy = lax.axis_index("gx"), lax.axis_index("gy")
    return lax.div(gy, NY), lax.rem(gy, NY), lax.div(gx, 2), lax.rem(gx, 2)


def dev(x, y, z, c):
    return (2 * z + c, NY * x + y)


def wrap(v, n):
    return lax.rem(v + n, n)


def rcopy(src, dst, send, recv, to):
    return pltpu.make_async_remote_copy(
        src_ref=src, dst_ref=dst, send_sem=send, recv_sem=recv, device_id=to, device_id_type=MESH
    )


def hails(x, y, z, c, partner, partner_self):
    barrier = pltpu.get_barrier_semaphore()

    def hail(to):
        pl.semaphore_signal(barrier, inc=1, device_id=to, device_id_type=MESH)

    hail(dev(wrap(x + 1, NX), y, z, c))
    hail(dev(wrap(x - 1, NX), y, z, c))
    hail(dev(x, y, wrap(z + 1, NZ), c))
    hail(dev(x, y, wrap(z - 1, NZ), c))
    for dy in range(1, NY):
        for flip in range(2):
            hail(dev(x, wrap(y + dy, NY), z, c if flip == 0 else 1 - c))
    hail(dev(x, y, z, 1 - c))

    @pl.when(jnp.logical_not(partner_self))
    def _():
        hail(partner)

    return lambda: pl.semaphore_wait(barrier, 11 + jnp.where(partner_self, 0, 1))


def f32(v):
    return v.astype(jnp.float32)


def bf16(v):
    return v.astype(jnp.bfloat16)


E_AT = {0: 0, -1: 1, 1: 2, 2: 3}
ORDER = [4, -2, -3, 3, 2, -1, 1, 0]


def kernel(
    g_coords, g_count, d_rows, d_coords, d_count,
    tok, gate, up, down, out,
    packed, w_all, relayed, xb, dgu, dd, acc, hid, part,
    ay_in1, ay_in2, ay_in3, ay_out, ay_sum, az_in, az_out,
    bz_in, bz_out, b_sum, by_in, by_out, final, send_sem, recv_sem,
):
    x, y, z, c = place()
    t = 1 - 2 * c
    partner = dev(lax.div(z, 2), y, 2 * x + c, lax.rem(z, 2))
    partner_self = z == 2 * x + c
    remote_partner = jnp.logical_not(partner_self)
    wait_all_here = hails(x, y, z, c, partner, partner_self)
    sibling = dev(x, y, z, 1 - c)
    x_up, x_down = dev(wrap(x + t, NX), y, z, c), dev(wrap(x - t, NX), y, z, c)
    y_up, y_down = dev(x, wrap(y + t, NY), z, c), dev(x, wrap(y - t, NY), z, c)
    z_up, z_down = dev(x, y, wrap(z + t, NZ), c), dev(x, y, wrap(z - t, NZ), c)
    sent, events, used = [], [], [0]

    def sem():
        used[0] += 1
        return used[0] - 1

    def go(src, dst, to):
        i = sem()
        copy = rcopy(src, dst, send_sem.at[i], recv_sem.at[i], to)
        copy.start()
        sent.append(copy)
        return copy

    def at(time, fn):
        events.append((time, len(events), fn))

    def run():
        for _, _, fn in sorted(events, key=lambda e: e[:2]):
            fn()
        events.clear()

    def xx(dx):
        return wrap(x + dx * t + NX, NX)

    def yy(dy):
        return wrap(y + dy * t + NY, NY)

    def zz(dz):
        return wrap(z + dz * t + NZ, NZ)

    def xblock(zi, yi, row, rows):
        start = pl.multiple_of(lax.rem(zi, 2) * TILE + row, 32)
        return xb.at[lax.div(zi, 2), pl.ds(start, rows), pl.ds(pl.multiple_of(yi * TILE, TILE), TILE)]

    low = lax.broadcasted_iota(jnp.int32, (BLOCK, BLOCK), 1) < HALF
    for s in range(CAP):
        g, u = f32(gate[s]), f32(up[s])
        packed[0, s * BLOCK : (s + 1) * BLOCK, :] = bf16(jnp.where(low, g, pltpu.roll(u, HALF, 1)))
        packed[1, s * BLOCK : (s + 1) * BLOCK, :] = bf16(jnp.where(low, pltpu.roll(g, HALF, 1), u))
    for s in range(CAPD):
        for h in range(2):
            packed[h, DOWN_AT + s * HALF : DOWN_AT + (s + 1) * HALF, :] = down[s, h * HALF : (h + 1) * HALF, :]
    slot_row = lax.broadcasted_iota(jnp.int32, (PIECE - META_AT, BLOCK), 0)
    ids = jnp.full((PIECE - META_AT, BLOCK), 99, jnp.int32)
    for s in range(CAP):
        spot = jnp.where(s < g_count[0], g_coords[0, s] * FB + g_coords[1, s], 99)
        ids = jnp.where(slot_row == s, spot, ids)
    for s in range(CAPD):
        kept = d_rows[d_coords[0, s], NY * x + y]
        spot = jnp.where(s < d_count[0], kept * DB + d_coords[1, s], 99)
        ids = jnp.where(slot_row == CAP + s, spot, ids)
    for h in range(2):
        packed[h, META_AT:PIECE, :] = bf16(f32(ids))

    wait_all_here()

    a_part, b_part = (0, ROWS_A), (ROWS_A, TILE - ROWS_A)

    lands = [sem() for _ in range(NY)]
    relay_at = sem()
    firsts = []

    def half(xi, yi, u):
        start = u * PART if isinstance(u, int) else pl.multiple_of(u * PART, 16)
        return w_all.at[xi, yi, pl.ds(start, PART)]

    def perm_part(rows):
        i = sem()
        src, mine = tok.at[pl.ds(*rows)], xblock(z, y, *rows)
        copy = rcopy(src, xblock(2 * x + c, y, *rows), send_sem.at[i], recv_sem.at[i], partner)
        here = pltpu.make_async_copy(src, mine, recv_sem.at[i])

        @pl.when(partner_self)
        def _():
            here.start()

        @pl.when(remote_partner)
        def _():
            copy.start()

        return copy, here

    perm_b = perm_part(b_part)
    for h in range(2):
        yd = 2 * c + h
        far = yd == wrap(y + 2, NY)
        for u in range(2):
            i = sem()
            src = packed.at[h, pl.ds(u * PART, PART)]
            same = jnp.logical_and(yd == y, c == u)
            there = rcopy(src, half(x, y, u), send_sem.at[i], recv_sem.at[lands[0] + y], dev(x, yd, z, u))
            hop = rcopy(src, relayed, send_sem.at[i], recv_sem.at[relay_at], dev(x, wrap(y + 1 - 2 * u, NY), z, u))

            @pl.when(far)
            def _(hop=hop):
                hop.start()

            @pl.when(same)
            def _(src=src, u=u):
                pltpu.make_async_copy(src, half(x, y, u), recv_sem.at[lands[0] + y]).start()

            @pl.when(jnp.logical_not(jnp.logical_or(far, same)))
            def _(there=there):
                there.start()

            firsts.append((same, there))
    perm_a = perm_part(a_part)

    def relay():
        pltpu.make_async_copy(relayed, relayed, recv_sem.at[relay_at]).wait()
        i = sem()
        copy = rcopy(relayed, half(x, yy(-1), c), send_sem.at[i], recv_sem.at[lands[0] + yy(-1)], y_up)
        copy.start()
        sent.append(copy)

    at(RELAY_STEP, relay)

    handed = []

    def hand(dx, dy):
        ref = half(xx(dx), yy(dy), c)
        handed.append(go(ref, ref, sibling))
        handed_at[-dx if abs(dx) == 1 else dx, -dy if abs(dy) == 1 else dy] = handed[-1]

    handed_at = {}

    def build(e, i):
        if i == 0:
            for dy in (0, 1, -1, 2):
                handed_at[e, dy].wait_recv()
        xa = xx(e)

        names = w_all[xa, i, META_AT : META_AT + 16, :]
        names = [jnp.broadcast_to(names[s : s + 1, :], (BLOCK, BLOCK)) for s in range(CAP + CAPD)]

        @pl.loop(0, DB)
        def _(r):
            for h in range(FB):
                w = jnp.zeros((BLOCK, BLOCK), jnp.bfloat16)
                for s in range(CAP):
                    hit = names[s] == (r * FB + h).astype(jnp.bfloat16)
                    w = jnp.where(hit, w_all[xa, i, s * BLOCK : (s + 1) * BLOCK, :], w)
                dgu[xa, pl.ds(pl.multiple_of(i * TILE + r * BLOCK, BLOCK), BLOCK), h * BLOCK : (h + 1) * BLOCK] = w

        for h in range(FB):
            for m in range(DB):
                w = jnp.zeros((HALF, BLOCK), jnp.bfloat16)
                for s in range(CAPD):
                    hit = names[CAP + s][:HALF] == jnp.bfloat16(h * DB + m)
                    at_row = DOWN_AT + s * HALF
                    w = jnp.where(hit, w_all[xa, i, at_row : at_row + HALF, :], w)
                dd[xa, i, h * HALF : (h + 1) * HALF, m * BLOCK : (m + 1) * BLOCK] = w

    for n, dy in enumerate((0, 1, -1, 2)):
        ring = {}

        def first(dy=dy, ring=ring):
            pltpu.make_async_copy(relayed, half(x, yy(dy), c), recv_sem.at[lands[0] + yy(dy)]).wait()
            ring["m1"] = go(half(x, yy(dy), c), half(x, yy(dy), c), x_up)
            ring["o1"] = go(half(x, yy(dy), c), half(x, yy(dy), c), x_down)
            hand(0, dy)

        def second(dy=dy, ring=ring):
            ring["m1"].wait_recv()
            ring["m2"] = go(half(xx(-1), yy(dy), c), half(xx(-1), yy(dy), c), x_up)
            hand(-1, dy)

        def third(dy=dy, ring=ring):
            ring["o1"].wait_recv()
            hand(1, dy)

        def fourth(dy=dy, ring=ring):
            ring["m2"].wait_recv()
            hand(2, dy)

        at(FIRST_AT[dy], first)
        at(SECOND_AT[dy], second)
        at(THIRD_AT[dy], third)
        at(FOURTH_AT[dy], fourth)
    for e in (0, -1, 1, 2):
        for i in range(NY):
            at(BUILD_AT[e, i], lambda e=e, i=i: build(e, i))

    def pass_on(dz, dy, part_rows, to):
        ref = xblock(zz(dz), yy(dy), *part_rows)
        return go(ref, ref, to)

    def along_y(dz, part_rows, time, then=None):
        ring = {}
        ring["m1"] = pass_on(dz, 0, part_rows, y_up)
        ring["o1"] = pass_on(dz, 0, part_rows, y_down)

        def second():
            ring["m1"].wait_recv()
            ring["m2"] = pass_on(dz, -1, part_rows, y_up)
            if then:
                then(-1)

        def third():
            ring["o1"].wait_recv()
            if then:
                then(1)

        def fourth():
            ring["m2"].wait_recv()
            if then:
                then(2)

        return second, third, fourth

    state = {}

    def z_start(dy):
        state["up", dy] = pass_on(0, dy, b_part, z_up)
        state["down", dy] = pass_on(0, dy, b_part, z_down)

    def z_up_step(k, dy):
        state["up", dy].wait_recv()
        if k < 4:
            state["up", dy] = pass_on(-k, dy, b_part, z_up)

    def z_down_step(k, dy):
        state["down", dy].wait_recv()
        if k < 3:
            state["down", dy] = pass_on(k, dy, b_part, z_down)

    def start_b():
        perm_b[1].wait()
        state["by"] = along_y(0, b_part, 0, z_start)
        z_start(0)

    def start_a():
        perm_a[1].wait()
        state["up"] = pass_on(0, 0, a_part, z_up)
        state["down"] = pass_on(0, 0, a_part, z_down)
        state["ay", 0] = along_y(0, a_part, 0)

    at(START_B, start_b)
    at(START_A, start_a)
    for k in range(1, 5):

        def a_up(k=k):
            state["up"].wait_recv()
            if k < 4:
                state["up"] = pass_on(-k, 0, a_part, z_up)
            state["ay", -k if k < 4 else 4] = along_y(-k, a_part, 0)

        def a_down(k=k):
            state["down"].wait_recv()
            if k < 3:
                state["down"] = pass_on(k, 0, a_part, z_down)
            state["ay", k] = along_y(k, a_part, 0)

        at(AUP_AT[k], a_up)
        if k < 4:
            at(ADOWN_AT[k], a_down)
    for dz in ORDER:
        for j in range(3):
            at((AY0_AT, AY1_AT, AY2_AT)[j][dz], lambda dz=dz, j=j: state["ay", dz][j]())
    for j in range(3):
        at((BY0_AT, BY1_AT, BY2_AT)[j], lambda j=j: state["by"][j]())
    for dy in (0, -1, 1, 2):
        for k in range(1, 5):
            at(ZUP_AT[k, dy], lambda k=k, dy=dy: z_up_step(k, dy))
            if k < 4:
                at(ZDOWN_AT[k, dy], lambda k=k, dy=dy: z_down_step(k, dy))

    def clear():
        acc[...] = jnp.zeros_like(acc)

        @pl.loop(0, NX * NY)
        def _(a):
            dd[lax.div(a, NY), lax.rem(a, NY), HID:, :] = jnp.zeros((2 * TILE - HID, TILE), jnp.bfloat16)

    at(-1, clear)

    def multiply(dz):
        xa = lax.div(zz(dz), 2)
        rows = pl.ds(pl.multiple_of(lax.rem(zz(dz), 2) * TILE, TILE), TILE)
        acc[rows, :] += jnp.dot(xb[xa, rows, :], dgu[xa], preferred_element_type=jnp.float32)

    for dz in ORDER:
        at(MUL_AT[dz], lambda dz=dz: multiply(dz))
    wide = lax.broadcasted_iota(jnp.int32, (TILE, BLOCK), 1) < HALF

    def hide(slice_at):
        rows = pl.ds(pl.multiple_of(slice_at * TILE, TILE), TILE)
        for pair in range(4):
            v = acc[rows, 2 * pair * BLOCK : (2 * pair + 1) * BLOCK]
            one = jax.nn.silu(v) * pltpu.roll(v, HALF, 1)
            if 2 * pair + 1 < FB:
                w = acc[rows, (2 * pair + 1) * BLOCK : (2 * pair + 2) * BLOCK]
                two = jax.nn.silu(pltpu.roll(w, HALF, 1)) * w
            else:
                two = jnp.zeros_like(one)
            hid[rows, pair * BLOCK : (pair + 1) * BLOCK] = bf16(jnp.where(wide, one, two))

    rows_a, rows_b = pl.ds(0, ROWS_A), pl.ds(ROWS_A, TILE - ROWS_A)
    DYS = (2, -1, 1, 0)
    first, direct, second = {}, {}, {}

    def begin(i):
        zi = zz(ORDER[i])
        first[i] = go(part.at[zi, yy(2), rows_a], ay_in1.at[i], y_up)
        direct[i] = go(part.at[zi, yy(-1), rows_a], ay_in3.at[i], y_down)

    def project(i):
        dz = ORDER[i]
        zi = zz(dz)
        mine_rows = hid[pl.ds(pl.multiple_of(lax.rem(zi, 2) * TILE, TILE), TILE), :]
        for dy in DYS:
            part[zi, yy(dy)] = bf16(
                jnp.dot(mine_rows, dd[lax.div(zi, 2), yy(dy)], preferred_element_type=jnp.float32)
            )
        for j, dy in enumerate(DYS):
            if dz == 4:
                state["bu", j] = go(part.at[zi, yy(dy), rows_b], bz_in.at[0, j], z_up)
            if dz == -3:
                state["bd", j] = go(part.at[zi, yy(dy), rows_b], bz_in.at[4, j], z_down)

    def a_first(i):
        first[i].wait_recv()
        ay_out[i] = bf16(f32(ay_in1[i]) + f32(part[zz(ORDER[i]), yy(1), rows_a]))
        second[i] = go(ay_out.at[i], ay_in2.at[i], y_up)

    def a_sum(i):
        direct[i].wait_recv()
        second[i].wait_recv()
        ay_sum[i] = bf16(f32(ay_in2[i]) + f32(ay_in3[i]) + f32(part[zz(ORDER[i]), y, rows_a]))
        if ORDER[i] == 4:
            state["au"] = go(ay_sum.at[i], az_in.at[0], z_up)
        if ORDER[i] == -3:
            state["ad"] = go(ay_sum.at[i], az_in.at[4], z_down)

    def chain_a_up(k):
        state["au"].wait_recv()
        if k < 4:
            az_out[k - 1] = bf16(f32(az_in[k - 1]) + f32(ay_sum[ORDER.index(4 - k)]))
            state["au"] = go(az_out.at[k - 1], az_in.at[k], z_up)

    def chain_a_down(k):
        state["ad"].wait_recv()
        if k < 3:
            az_out[k + 2] = bf16(f32(az_in[k + 3]) + f32(ay_sum[ORDER.index(k - 3)]))
            state["ad"] = go(az_out.at[k + 2], az_in.at[k + 4], z_down)

    def chain_b_up(k, j):
        state["bu", j].wait_recv()
        if k < 4:
            bz_out[k - 1, j] = bf16(f32(bz_in[k - 1, j]) + f32(part[zz(4 - k), yy(DYS[j]), rows_b]))
            state["bu", j] = go(bz_out.at[k - 1, j], bz_in.at[k, j], z_up)

    def chain_b_down(k, j):
        state["bd", j].wait_recv()
        if k < 3:
            bz_out[k + 2, j] = bf16(f32(bz_in[k + 3, j]) + f32(part[zz(k - 3), yy(DYS[j]), rows_b]))
            state["bd", j] = go(bz_out.at[k + 2, j], bz_in.at[k + 4, j], z_down)

    def b_end(j):
        b_sum[j] = bf16(f32(bz_in[3, j]) + f32(bz_in[6, j]) + f32(part[z, yy(DYS[j]), rows_b]))
        if j == 0:
            state["by1"] = go(b_sum.at[0], by_in.at[0], y_up)
        if j == 1:
            state["by3"] = go(b_sum.at[1], by_in.at[2], y_down)

    def b_relay():
        state["by1"].wait_recv()
        by_out[...] = bf16(f32(by_in[0]) + f32(b_sum[2]))
        state["by2"] = go(by_out, by_in.at[1], y_up)

    lasts = []

    def deliver(rows):
        i = sem()
        copy = rcopy(final.at[rows], out.at[rows], send_sem.at[i], recv_sem.at[i], partner)
        here = pltpu.make_async_copy(final.at[rows], out.at[rows], recv_sem.at[i])

        @pl.when(partner_self)
        def _():
            here.start()

        @pl.when(remote_partner)
        def _():
            copy.start()

        lasts.append((copy, here))

    def b_last():
        state["by3"].wait_recv()
        state["by2"].wait_recv()
        final[rows_b] = bf16(f32(by_in[1]) + f32(by_in[2]) + f32(b_sum[3]))
        deliver(rows_b)

    def a_last():
        final[rows_a] = bf16(f32(az_in[3]) + f32(az_in[6]) + f32(ay_sum[7]))
        deliver(rows_a)

    even_done = max(MUL_AT[dz] for dz in ORDER if dz % 2 == 0)

    def early():
        hide(lax.rem(z, 2))
        for i in range(2):
            project(i)
            begin(i)

    at(even_done + 0.5, early)
    last_mul = max(MUL_AT.values())
    rs = last_mul + 1
    f, s_at, d = RT["f"], RT["s"], RT["d"]
    at(rs - 0.5, lambda: hide(lax.rem(z + 1, 2)))
    for i in range(8):
        if i >= 2:
            at(rs + 4.2 + 0.45 * (i - 2), lambda i=i: project(i))
            at(rs + max(f + d * (i - 2), 4.2 + 0.45 * (i - 2)) + 0.01, lambda i=i: begin(i))
        at(rs + f + d * i, lambda i=i: a_first(i))
        at(rs + s_at + d * i, lambda i=i: a_sum(i))
    for j in range(4):
        for k in range(1, 5):
            up = rs + RT["b"] + 0.7 * j + RT["bd"] * (k - 1)
            at(up, lambda k=k, j=j: chain_b_up(k, j))
            if k < 4:
                at(up + RT["bx"], lambda k=k, j=j: chain_b_down(k, j))
        at(up + 0.1, lambda j=j: b_end(j))
    at(up + RT["y"], b_relay)
    at(up + 2 * RT["y"], b_last)
    slot = {dz: rs + s_at + d * i + 0.1 for i, dz in enumerate(ORDER)}
    up, down = slot[4], slot[-3]
    for k in range(1, 5):
        up = max(slot[4 - k], up + RT["z"])
        at(up, lambda k=k: chain_a_up(k))
        if k < 4:
            down = max(slot[k - 3], down + RT["z"])
            at(down, lambda k=k: chain_a_down(k))
    at(max(up, down) + 0.1, a_last)
    run()

    for copy in sent:
        copy.wait_send()
    for same, copy in firsts:

        @pl.when(jnp.logical_not(same))
        def _(copy=copy):
            copy.wait_send()

    @pl.when(remote_partner)
    def _():
        perm_a[0].wait_send()
        perm_b[0].wait_send()

    for copy, here in lasts:
        here.wait()

        @pl.when(remote_partner)
        def _(copy=copy):
            copy.wait_send()


SEMS = 200
START_B = 1
START_A = 9
FIRST_AT = {0: 0, 1: 2, -1: 10, 2: 16}
RELAY_STEP = 3
SECOND_AT = {0: 4, 1: 18, -1: 43, 2: 50}
THIRD_AT = {0: 5, 1: 19, -1: 34, 2: 44}
ZUP_AT = {(1, 0): 6, (2, 0): 12, (1, 1): 14, (1, -1): 22, (3, 0): 28, (2, 1): 30, (2, -1): 38, (1, 2): 40, (3, 1): 42, (3, -1): 52, (2, 2): 55, (3, 2): 64, (4, 0): 82, (4, 1): 83, (4, -1): 84, (4, 2): 85}
ZDOWN_AT = {(1, 0): 7, (2, 0): 13, (1, 1): 15, (1, -1): 24, (2, 1): 31, (1, 2): 39, (2, -1): 41, (2, 2): 48, (3, 0): 95, (3, 1): 96, (3, -1): 97, (3, 2): 98}
BY1_AT = 8
BY0_AT = 11
AUP_AT = {1: 17, 2: 35, 3: 47, 4: 62}
ADOWN_AT = {1: 20, 2: 36, 3: 46}
AY0_AT = {0: 21, -1: 32, 1: 37, -2: 45, 2: 49, 3: 63, -3: 66, 4: 68}
BY2_AT = 23
BUILD_AT = {(0, 0): 25, (0, 1): 26, (0, 2): 27, (0, 3): 29, (-1, 0): 51, (-1, 1): 53, (-1, 2): 54, (-1, 3): 56, (1, 0): 57, (1, 1): 58, (1, 2): 60, (1, 3): 61, (2, 0): 69, (2, 1): 70, (2, 2): 71, (2, 3): 72}
FOURTH_AT = {0: 33, 1: 59, -1: 65, 2: 67}
AY1_AT = {0: 73, -2: 76, 2: 79, 4: 86, -1: 89, 1: 92, 3: 99, -3: 102}
AY2_AT = {0: 74, -2: 77, 2: 80, 4: 87, -1: 90, 1: 93, 3: 100, -3: 103}
MUL_AT = {0: 75, -2: 78, 2: 81, 4: 88, -1: 91, 1: 94, 3: 101, -3: 104}
RT = {"f": 3.9, "s": 7.0, "d": 2.7, "b": 5.0, "bd": 4.8, "bx": 2.5, "y": 2.7, "z": 2.9}


def body(
    tokens, gate_blocks, up_blocks, gate_coords, gate_count,
    down_blocks, down_rows, down_coords, down_count,
):
    vmem, smem = pl.BlockSpec(memory_space=pltpu.VMEM), pl.BlockSpec(memory_space=pltpu.SMEM)
    rb = TILE - ROWS_A
    bf = lambda *s: pltpu.VMEM(s, jnp.bfloat16)
    return pl.pallas_call(
        kernel,
        out_shape=jax.ShapeDtypeStruct((TILE, TILE), jnp.bfloat16),
        in_specs=[smem] * 5 + [vmem] * 4,
        out_specs=vmem,
        scratch_shapes=[
            bf(2, PIECE, BLOCK), bf(NX, NY, PIECE, BLOCK), bf(PART, BLOCK),
            bf(NX, 2 * TILE, WIDE), bf(NX, WIDE, FB * BLOCK), bf(NX, NY, 2 * TILE, TILE),
            pltpu.VMEM((2 * TILE, FB * BLOCK), jnp.float32), bf(2 * TILE, 2 * TILE),
            bf(NZ, NY, TILE, TILE),
            bf(8, ROWS_A, TILE), bf(8, ROWS_A, TILE), bf(8, ROWS_A, TILE), bf(8, ROWS_A, TILE), bf(8, ROWS_A, TILE),
            bf(7, ROWS_A, TILE), bf(5, ROWS_A, TILE),
            bf(7, NY, rb, TILE), bf(5, NY, rb, TILE), bf(NY, rb, TILE), bf(3, rb, TILE), bf(rb, TILE),
            bf(TILE, TILE),
            pltpu.SemaphoreType.DMA((SEMS,)),
            pltpu.SemaphoreType.DMA((SEMS,)),
        ],
        compiler_params=pltpu.CompilerParams(
            collective_id=0, has_side_effects=True, vmem_limit_bytes=58 * 2**20
        ),
    )(
        gate_coords[0, 0].T, gate_count.reshape(-1), down_rows[0].T,
        down_coords[0, 0].T, down_count.reshape(-1),
        tokens, gate_blocks[0, 0], up_blocks[0, 0], down_blocks[0, 0],
    )


def solution(mesh):
    return jax.shard_map(
        body,
        mesh=mesh,
        in_specs=(
            P("gx", "gy"),
            P("gy", "gx", None, None, None),
            P("gy", "gx", None, None, None),
            P("gy", "gx", None, None),
            P("gy", "gx"),
            P("gx", "gy", None, None, None),
            P("gx", None, None),
            P("gx", "gy", None, None),
            P("gx", "gy"),
        ),
        out_specs=P("gx", "gy"),
        check_vma=False,
    )
```

```python
import jax
import jax.numpy as jnp
from jax import lax
from jax.experimental import pallas as pl
from jax.experimental.pallas import tpu as pltpu
from jax.sharding import PartitionSpec as P

MESH = pl.DeviceIdType.MESH
BLOCK = 128
HALF = 64
NX, NY, NZ = 4, 4, 8
DB, FB = 2, 7
CAP, CAPD = 10, 6
TILE = 256
GU = CAP * BLOCK
DOWN_AT = GU
META_AT = GU + CAPD * HALF
PIECE = META_AT + 32
PART = PIECE // 2
WIDE = NY * TILE
HID = FB * HALF
ROWS_A = 160


def place():
    gx, gy = lax.axis_index("gx"), lax.axis_index("gy")
    return lax.div(gy, NY), lax.rem(gy, NY), lax.div(gx, 2), lax.rem(gx, 2)


def dev(x, y, z, c):
    return (2 * z + c, NY * x + y)


def wrap(v, n):
    return lax.rem(v + n, n)


def rcopy(src, dst, send, recv, to):
    return pltpu.make_async_remote_copy(
        src_ref=src, dst_ref=dst, send_sem=send, recv_sem=recv, device_id=to, device_id_type=MESH
    )


def z_of(x, c):
    return lax.rem(2 * x + 3 * c, NZ)


def x_of(z):
    return lax.div(lax.rem(z + 5 * lax.rem(z, 2), NZ), 2)


def hails(x, y, z, c, partner, partner_self):
    barrier = pltpu.get_barrier_semaphore()

    def hail(to):
        pl.semaphore_signal(barrier, inc=1, device_id=to, device_id_type=MESH)

    hail(dev(wrap(x + 1, NX), y, z, c))
    hail(dev(wrap(x - 1, NX), y, z, c))
    hail(dev(x, y, wrap(z + 1, NZ), c))
    hail(dev(x, y, wrap(z - 1, NZ), c))
    for dy in range(1, NY):
        for flip in range(2):
            hail(dev(x, wrap(y + dy, NY), z, c if flip == 0 else 1 - c))
    hail(dev(x, y, z, 1 - c))

    @pl.when(jnp.logical_not(partner_self))
    def _():
        hail(partner)

    return lambda: pl.semaphore_wait(barrier, 11 + jnp.where(partner_self, 0, 1))


def f32(v):
    return v.astype(jnp.float32)


def bf16(v):
    return v.astype(jnp.bfloat16)


E_AT = {0: 0, -1: 1, 1: 2, 2: 3}
ORDER = [4, -2, -3, 3, 2, -1, 1, 0]


def kernel(
    g_coords, g_count, d_rows, d_coords, d_count,
    tok, gate, up, down, out,
    packed, w_all, relayed, xb, dgu, dd, acc, hid, part,
    ay_in1, ay_in2, ay_in3, ay_out, ay_sum, az_in, az_out,
    bz_in, bz_out, b_sum, by_in, by_out, final, send_sem, recv_sem,
):
    x, y, z, c = place()
    t = 1 - 2 * c
    partner = dev(x_of(z), y, z_of(x, c), lax.rem(z, 2))
    partner_self = z == z_of(x, c)
    remote_partner = jnp.logical_not(partner_self)
    wait_all_here = hails(x, y, z, c, partner, partner_self)
    sibling = dev(x, y, z, 1 - c)
    x_up, x_down = dev(wrap(x + t, NX), y, z, c), dev(wrap(x - t, NX), y, z, c)
    y_up, y_down = dev(x, wrap(y + t, NY), z, c), dev(x, wrap(y - t, NY), z, c)
    z_up, z_down = dev(x, y, wrap(z + t, NZ), c), dev(x, y, wrap(z - t, NZ), c)
    sent, events, used = [], [], [0]

    def sem():
        used[0] += 1
        return used[0] - 1

    def go(src, dst, to):
        i = sem()
        copy = rcopy(src, dst, send_sem.at[i], recv_sem.at[i], to)
        copy.start()
        sent.append(copy)
        return copy

    def at(time, fn):
        events.append((time, len(events), fn))

    def run():
        for _, _, fn in sorted(events, key=lambda e: e[:2]):
            fn()
        events.clear()

    def xx(dx):
        return wrap(x + dx * t + NX, NX)

    def yy(dy):
        return wrap(y + dy * t + NY, NY)

    def zz(dz):
        return wrap(z + dz * t + NZ, NZ)

    def xblock(zi, yi, row, rows):
        start = pl.multiple_of(lax.rem(zi, 2) * TILE + row, 32)
        return xb.at[x_of(zi), pl.ds(start, rows), pl.ds(pl.multiple_of(yi * TILE, TILE), TILE)]

    low = lax.broadcasted_iota(jnp.int32, (BLOCK, BLOCK), 1) < HALF
    for s in range(CAP):
        g, u = f32(gate[s]), f32(up[s])
        packed[0, s * BLOCK : (s + 1) * BLOCK, :] = bf16(jnp.where(low, g, pltpu.roll(u, HALF, 1)))
        packed[1, s * BLOCK : (s + 1) * BLOCK, :] = bf16(jnp.where(low, pltpu.roll(g, HALF, 1), u))
    for s in range(CAPD):
        for h in range(2):
            packed[h, DOWN_AT + s * HALF : DOWN_AT + (s + 1) * HALF, :] = down[s, h * HALF : (h + 1) * HALF, :]
    slot_row = lax.broadcasted_iota(jnp.int32, (PIECE - META_AT, BLOCK), 0)
    ids = jnp.full((PIECE - META_AT, BLOCK), 99, jnp.int32)
    for s in range(CAP):
        spot = jnp.where(s < g_count[0], g_coords[0, s] * FB + g_coords[1, s], 99)
        ids = jnp.where(slot_row == s, spot, ids)
    for s in range(CAPD):
        kept = d_rows[d_coords[0, s], NY * x + y]
        spot = jnp.where(s < d_count[0], kept * DB + d_coords[1, s], 99)
        ids = jnp.where(slot_row == CAP + s, spot, ids)
    for h in range(2):
        packed[h, META_AT:PIECE, :] = bf16(f32(ids))

    wait_all_here()

    a_part, b_part = (0, ROWS_A), (ROWS_A, TILE - ROWS_A)

    lands = [sem() for _ in range(NY)]
    relay_at = sem()
    firsts = []

    def half(xi, yi, u):
        start = u * PART if isinstance(u, int) else pl.multiple_of(u * PART, 16)
        return w_all.at[xi, yi, pl.ds(start, PART)]

    def perm_part(rows):
        i = sem()
        src, mine = tok.at[pl.ds(*rows)], xblock(z, y, *rows)
        copy = rcopy(src, xblock(z_of(x, c), y, *rows), send_sem.at[i], recv_sem.at[i], partner)
        here = pltpu.make_async_copy(src, mine, recv_sem.at[i])

        @pl.when(partner_self)
        def _():
            here.start()

        @pl.when(remote_partner)
        def _():
            copy.start()

        return copy, here

    perm_b = perm_part(b_part)
    for h in range(2):
        yd = 2 * c + h
        far = yd == wrap(y + 2, NY)
        for u in range(2):
            i = sem()
            src = packed.at[h, pl.ds(u * PART, PART)]
            same = jnp.logical_and(yd == y, c == u)
            there = rcopy(src, half(x, y, u), send_sem.at[i], recv_sem.at[lands[0] + y], dev(x, yd, z, u))
            hop = rcopy(src, relayed, send_sem.at[i], recv_sem.at[relay_at], dev(x, wrap(y + 1 - 2 * u, NY), z, u))

            @pl.when(far)
            def _(hop=hop):
                hop.start()

            @pl.when(same)
            def _(src=src, u=u):
                pltpu.make_async_copy(src, half(x, y, u), recv_sem.at[lands[0] + y]).start()

            @pl.when(jnp.logical_not(jnp.logical_or(far, same)))
            def _(there=there):
                there.start()

            firsts.append((same, there))
    perm_a = perm_part(a_part)

    def relay():
        pltpu.make_async_copy(relayed, relayed, recv_sem.at[relay_at]).wait()
        i = sem()
        copy = rcopy(relayed, half(x, yy(-1), c), send_sem.at[i], recv_sem.at[lands[0] + yy(-1)], y_up)
        copy.start()
        sent.append(copy)

    at(RELAY_STEP, relay)

    handed = []

    def hand(dx, dy):
        ref = half(xx(dx), yy(dy), c)
        handed.append(go(ref, ref, sibling))
        handed_at[-dx if abs(dx) == 1 else dx, -dy if abs(dy) == 1 else dy] = handed[-1]

    handed_at = {}

    def build(e, dy):
        handed_at[e, dy].wait_recv()
        xa, i = xx(e), yy(dy)

        names = w_all[xa, i, META_AT : META_AT + 16, :]
        names = [jnp.broadcast_to(names[s : s + 1, :], (BLOCK, BLOCK)) for s in range(CAP + CAPD)]

        @pl.loop(0, DB)
        def _(r):
            for h in range(FB):
                w = jnp.zeros((BLOCK, BLOCK), jnp.bfloat16)
                for s in range(CAP):
                    hit = names[s] == (r * FB + h).astype(jnp.bfloat16)
                    w = jnp.where(hit, w_all[xa, i, s * BLOCK : (s + 1) * BLOCK, :], w)
                dgu[xa, pl.ds(pl.multiple_of(i * TILE + r * BLOCK, BLOCK), BLOCK), h * BLOCK : (h + 1) * BLOCK] = w

        for h in range(FB):
            for m in range(DB):
                w = jnp.zeros((HALF, BLOCK), jnp.bfloat16)
                for s in range(CAPD):
                    hit = names[CAP + s][:HALF] == jnp.bfloat16(h * DB + m)
                    at_row = DOWN_AT + s * HALF
                    w = jnp.where(hit, w_all[xa, i, at_row : at_row + HALF, :], w)
                dd[xa, i, h * HALF : (h + 1) * HALF, m * BLOCK : (m + 1) * BLOCK] = w

    for n, dy in enumerate((0, 1, -1, 2)):
        ring = {}

        def first(dy=dy, ring=ring):
            pltpu.make_async_copy(relayed, half(x, yy(dy), c), recv_sem.at[lands[0] + yy(dy)]).wait()
            ring["m1"] = go(half(x, yy(dy), c), half(x, yy(dy), c), x_up)
            ring["o1"] = go(half(x, yy(dy), c), half(x, yy(dy), c), x_down)
            hand(0, dy)

        def second(dy=dy, ring=ring):
            ring["m1"].wait_recv()
            ring["m2"] = go(half(xx(-1), yy(dy), c), half(xx(-1), yy(dy), c), x_up)
            hand(-1, dy)

        def third(dy=dy, ring=ring):
            ring["o1"].wait_recv()
            hand(1, dy)

        def fourth(dy=dy, ring=ring):
            ring["m2"].wait_recv()
            hand(2, dy)

        at(FIRST_AT[dy], first)
        at(SECOND_AT[dy], second)
        at(THIRD_AT[dy], third)
        at(FOURTH_AT[dy], fourth)
    for e in (0, -1, 1, 2):
        for i in (0, 1, -1, 2):
            at(BUILD_AT[e, i], lambda e=e, i=i: build(e, i))

    def pass_on(dz, dy, part_rows, to):
        ref = xblock(zz(dz), yy(dy), *part_rows)
        return go(ref, ref, to)

    def along_y(dz, part_rows, time, then=None):
        ring = {}
        ring["m1"] = pass_on(dz, 0, part_rows, y_up)
        ring["o1"] = pass_on(dz, 0, part_rows, y_down)

        def second():
            ring["m1"].wait_recv()
            ring["m2"] = pass_on(dz, -1, part_rows, y_up)
            if then:
                then(-1)

        def third():
            ring["o1"].wait_recv()
            if then:
                then(1)

        def fourth():
            ring["m2"].wait_recv()
            if then:
                then(2)

        return second, third, fourth

    state = {}

    def z_start(dy):
        state["up", dy] = pass_on(0, dy, b_part, z_up)
        state["down", dy] = pass_on(0, dy, b_part, z_down)

    def z_up_step(k, dy):
        state["up", dy].wait_recv()
        if k < 4:
            state["up", dy] = pass_on(-k, dy, b_part, z_up)

    def z_down_step(k, dy):
        state["down", dy].wait_recv()
        if k < 3:
            state["down", dy] = pass_on(k, dy, b_part, z_down)

    def start_b():
        perm_b[1].wait()
        state["by"] = along_y(0, b_part, 0, z_start)
        z_start(0)

    def start_a():
        perm_a[1].wait()
        state["up"] = pass_on(0, 0, a_part, z_up)
        state["down"] = pass_on(0, 0, a_part, z_down)
        state["ay", 0] = along_y(0, a_part, 0)

    at(START_B, start_b)
    at(START_A, start_a)
    for k in range(1, 5):

        def a_up(k=k):
            state["up"].wait_recv()
            if k < 4:
                state["up"] = pass_on(-k, 0, a_part, z_up)
            state["ay", -k if k < 4 else 4] = along_y(-k, a_part, 0)

        def a_down(k=k):
            state["down"].wait_recv()
            if k < 3:
                state["down"] = pass_on(k, 0, a_part, z_down)
            state["ay", k] = along_y(k, a_part, 0)

        at(AUP_AT[k], a_up)
        if k < 4:
            at(ADOWN_AT[k], a_down)
    for dz in ORDER:
        for j in range(3):
            at((AY0_AT, AY1_AT, AY2_AT)[j][dz], lambda dz=dz, j=j: state["ay", dz][j]())
    for j in range(3):
        at((BY0_AT, BY1_AT, BY2_AT)[j], lambda j=j: state["by"][j]())
    for dy in (0, -1, 1, 2):
        for k in range(1, 5):
            at(ZUP_AT[k, dy], lambda k=k, dy=dy: z_up_step(k, dy))
            if k < 4:
                at(ZDOWN_AT[k, dy], lambda k=k, dy=dy: z_down_step(k, dy))

    def clear():
        acc[...] = jnp.zeros_like(acc)

        @pl.loop(0, NX * NY)
        def _(a):
            dd[lax.div(a, NY), lax.rem(a, NY), HID:, :] = jnp.zeros((2 * TILE - HID, TILE), jnp.bfloat16)

    at(-1, clear)

    def multiply(dz):
        xa = x_of(zz(dz))
        rows = pl.ds(pl.multiple_of(lax.rem(zz(dz), 2) * TILE, TILE), TILE)
        acc[rows, :] += jnp.dot(xb[xa, rows, :], dgu[xa], preferred_element_type=jnp.float32)

    def multiply_if(dz, last):
        here = x_of(zz(dz)) == xx(2)

        @pl.when(here if last else jnp.logical_not(here))
        def _():
            multiply(dz)

    for dz in ORDER:
        if dz in (0, -2, 2):
            at(EARLY_AT[dz], lambda dz=dz: multiply_if(dz, False))
            at(MUL_AT[dz], lambda dz=dz: multiply_if(dz, True))
        else:
            at(MUL_AT[dz], lambda dz=dz: multiply(dz))
    wide = lax.broadcasted_iota(jnp.int32, (TILE, BLOCK), 1) < HALF

    def hide(slice_at):
        rows = pl.ds(pl.multiple_of(slice_at * TILE, TILE), TILE)
        for pair in range(4):
            v = acc[rows, 2 * pair * BLOCK : (2 * pair + 1) * BLOCK]
            one = jax.nn.silu(v) * pltpu.roll(v, HALF, 1)
            if 2 * pair + 1 < FB:
                w = acc[rows, (2 * pair + 1) * BLOCK : (2 * pair + 2) * BLOCK]
                two = jax.nn.silu(pltpu.roll(w, HALF, 1)) * w
            else:
                two = jnp.zeros_like(one)
            hid[rows, pair * BLOCK : (pair + 1) * BLOCK] = bf16(jnp.where(wide, one, two))

    rows_a, rows_b = pl.ds(0, ROWS_A), pl.ds(ROWS_A, TILE - ROWS_A)
    DYS = (2, -1, 1, 0)
    first, direct, second = {}, {}, {}

    def begin(i):
        zi = zz(ORDER[i])
        first[i] = go(part.at[zi, yy(2), rows_a], ay_in1.at[i], y_up)
        direct[i] = go(part.at[zi, yy(-1), rows_a], ay_in3.at[i], y_down)

    def project(i):
        dz = ORDER[i]
        zi = zz(dz)
        mine_rows = hid[pl.ds(pl.multiple_of(lax.rem(zi, 2) * TILE, TILE), TILE), :]
        for dy in DYS:
            part[zi, yy(dy)] = bf16(
                jnp.dot(mine_rows, dd[x_of(zi), yy(dy)], preferred_element_type=jnp.float32)
            )
        for j, dy in enumerate(DYS):
            if dz == 4:
                state["bu", j] = go(part.at[zi, yy(dy), rows_b], bz_in.at[0, j], z_up)
            if dz == -3:
                state["bd", j] = go(part.at[zi, yy(dy), rows_b], bz_in.at[4, j], z_down)

    def a_first(i):
        first[i].wait_recv()
        ay_out[i] = bf16(f32(ay_in1[i]) + f32(part[zz(ORDER[i]), yy(1), rows_a]))
        second[i] = go(ay_out.at[i], ay_in2.at[i], y_up)

    def a_sum(i):
        direct[i].wait_recv()
        second[i].wait_recv()
        ay_sum[i] = bf16(f32(ay_in2[i]) + f32(ay_in3[i]) + f32(part[zz(ORDER[i]), y, rows_a]))
        if ORDER[i] == 4:
            state["au"] = go(ay_sum.at[i], az_in.at[0], z_up)
        if ORDER[i] == -3:
            state["ad"] = go(ay_sum.at[i], az_in.at[4], z_down)

    def chain_a_up(k):
        state["au"].wait_recv()
        if k < 4:
            az_out[k - 1] = bf16(f32(az_in[k - 1]) + f32(ay_sum[ORDER.index(4 - k)]))
            state["au"] = go(az_out.at[k - 1], az_in.at[k], z_up)

    def chain_a_down(k):
        state["ad"].wait_recv()
        if k < 3:
            az_out[k + 2] = bf16(f32(az_in[k + 3]) + f32(ay_sum[ORDER.index(k - 3)]))
            state["ad"] = go(az_out.at[k + 2], az_in.at[k + 4], z_down)

    def chain_b_up(k, j):
        state["bu", j].wait_recv()
        if k < 4:
            bz_out[k - 1, j] = bf16(f32(bz_in[k - 1, j]) + f32(part[zz(4 - k), yy(DYS[j]), rows_b]))
            state["bu", j] = go(bz_out.at[k - 1, j], bz_in.at[k, j], z_up)

    def chain_b_down(k, j):
        state["bd", j].wait_recv()
        if k < 3:
            bz_out[k + 2, j] = bf16(f32(bz_in[k + 3, j]) + f32(part[zz(k - 3), yy(DYS[j]), rows_b]))
            state["bd", j] = go(bz_out.at[k + 2, j], bz_in.at[k + 4, j], z_down)

    def b_end(j):
        b_sum[j] = bf16(f32(bz_in[3, j]) + f32(bz_in[6, j]) + f32(part[z, yy(DYS[j]), rows_b]))
        if j == 0:
            state["by1"] = go(b_sum.at[0], by_in.at[0], y_up)
        if j == 1:
            state["by3"] = go(b_sum.at[1], by_in.at[2], y_down)

    def b_relay():
        state["by1"].wait_recv()
        by_out[...] = bf16(f32(by_in[0]) + f32(b_sum[2]))
        state["by2"] = go(by_out, by_in.at[1], y_up)

    lasts = []

    def deliver(rows):
        i = sem()
        copy = rcopy(final.at[rows], out.at[rows], send_sem.at[i], recv_sem.at[i], partner)
        here = pltpu.make_async_copy(final.at[rows], out.at[rows], recv_sem.at[i])

        @pl.when(partner_self)
        def _():
            here.start()

        @pl.when(remote_partner)
        def _():
            copy.start()

        lasts.append((copy, here))

    def b_last():
        state["by3"].wait_recv()
        state["by2"].wait_recv()
        final[rows_b] = bf16(f32(by_in[1]) + f32(by_in[2]) + f32(b_sum[3]))
        deliver(rows_b)

    def a_last():
        final[rows_a] = bf16(f32(az_in[3]) + f32(az_in[6]) + f32(ay_sum[7]))
        deliver(rows_a)

    even_done = max(MUL_AT[dz] for dz in ORDER if dz % 2 == 0)

    def early():
        hide(lax.rem(z, 2))
        for i in range(2):
            project(i)
            begin(i)

    at(even_done + 0.5, early)
    last_mul = max(MUL_AT.values())
    rs = last_mul + 1
    f, s_at, d = RT["f"], RT["s"], RT["d"]
    at(rs - 0.5, lambda: hide(lax.rem(z + 1, 2)))
    for i in range(8):
        if i >= 2:
            at(rs + 4.2 + 0.45 * (i - 2), lambda i=i: project(i))
            at(rs + max(f + d * (i - 2), 4.2 + 0.45 * (i - 2)) + 0.01, lambda i=i: begin(i))
        at(rs + f + d * i, lambda i=i: a_first(i))
        at(rs + s_at + d * i, lambda i=i: a_sum(i))
    for j in range(4):
        for k in range(1, 5):
            up = rs + RT["b"] + 0.7 * j + RT["bd"] * (k - 1)
            at(up, lambda k=k, j=j: chain_b_up(k, j))
            if k < 4:
                at(up + RT["bx"], lambda k=k, j=j: chain_b_down(k, j))
        at(up + 0.1, lambda j=j: b_end(j))
    at(up + RT["y"], b_relay)
    at(up + 2 * RT["y"], b_last)
    slot = {dz: rs + s_at + d * i + 0.1 for i, dz in enumerate(ORDER)}
    up, down = slot[4], slot[-3]
    for k in range(1, 5):
        up = max(slot[4 - k], up + RT["z"])
        at(up, lambda k=k: chain_a_up(k))
        if k < 4:
            down = max(slot[k - 3], down + RT["z"])
            at(down, lambda k=k: chain_a_down(k))
    at(max(up, down) + 0.1, a_last)
    run()

    for copy in sent:
        copy.wait_send()
    for same, copy in firsts:

        @pl.when(jnp.logical_not(same))
        def _(copy=copy):
            copy.wait_send()

    @pl.when(remote_partner)
    def _():
        perm_a[0].wait_send()
        perm_b[0].wait_send()

    for copy, here in lasts:
        here.wait()

        @pl.when(remote_partner)
        def _(copy=copy):
            copy.wait_send()


SEMS = 200
START_B = 2
START_A = 7
FIRST_AT = {0: 0, 1: 3, -1: 13, 2: 23}
BUILD_AT = {(0, 0): 1, (1, 0): 11, (-1, 0): 12, (0, -1): 14, (0, 1): 18, (0, 2): 28, (1, -1): 40, (2, 0): 42, (-1, 1): 45, (-1, -1): 53, (1, 1): 55, (-1, 2): 59, (1, 2): 62, (2, -1): 76, (2, 1): 78, (2, 2): 81}
RELAY_STEP = 4
ZUP_AT = {(1, 0): 5, (2, 0): 15, (1, 1): 21, (3, 0): 26, (1, -1): 29, (2, 1): 35, (2, -1): 43, (1, 2): 47, (3, 1): 54, (3, -1): 56, (2, 2): 60, (3, 2): 71, (4, 0): 85, (4, -1): 86, (4, 1): 87, (4, 2): 89}
ZDOWN_AT = {(1, 0): 6, (2, 0): 16, (1, 1): 22, (1, -1): 30, (2, 1): 36, (2, -1): 41, (1, 2): 44, (2, 2): 57, (3, 0): 101, (3, 1): 102, (3, -1): 103, (3, 2): 105}
SECOND_AT = {0: 8, 1: 24, -1: 51, 2: 58}
THIRD_AT = {0: 9, 1: 25, -1: 39, 2: 52}
BY1_AT = 10
BY0_AT = 17
AUP_AT = {1: 19, 2: 32, 3: 50, 4: 61}
ADOWN_AT = {1: 20, 2: 33, 3: 48}
AY0_AT = {0: 27, -1: 34, 1: 37, -2: 46, 2: 49, 3: 70, -3: 77, 4: 79}
BY2_AT = 31
FOURTH_AT = {0: 38, 1: 66, -1: 75, 2: 80}
AY1_AT = {0: 63, -2: 67, 2: 72, 4: 88, -1: 92, 1: 95, -3: 98, 3: 104}
AY2_AT = {0: 64, -2: 68, 2: 73, 4: 90, -1: 93, 1: 96, -3: 99, 3: 106}
EARLY_AT = {0: 65, -2: 69, 2: 74}
MUL_AT = {0: 82, -2: 83, 2: 84, 4: 91, -1: 94, 1: 97, -3: 100, 3: 107}
RT = {"f": 3.9, "s": 7.0, "d": 2.7, "b": 5.0, "bd": 4.8, "bx": 2.5, "y": 2.7, "z": 2.9}


def body(
    tokens, gate_blocks, up_blocks, gate_coords, gate_count,
    down_blocks, down_rows, down_coords, down_count,
):
    vmem, smem = pl.BlockSpec(memory_space=pltpu.VMEM), pl.BlockSpec(memory_space=pltpu.SMEM)
    rb = TILE - ROWS_A
    bf = lambda *s: pltpu.VMEM(s, jnp.bfloat16)
    return pl.pallas_call(
        kernel,
        out_shape=jax.ShapeDtypeStruct((TILE, TILE), jnp.bfloat16),
        in_specs=[smem] * 5 + [vmem] * 4,
        out_specs=vmem,
        scratch_shapes=[
            bf(2, PIECE, BLOCK), bf(NX, NY, PIECE, BLOCK), bf(PART, BLOCK),
            bf(NX, 2 * TILE, WIDE), bf(NX, WIDE, FB * BLOCK), bf(NX, NY, 2 * TILE, TILE),
            pltpu.VMEM((2 * TILE, FB * BLOCK), jnp.float32), bf(2 * TILE, 2 * TILE),
            bf(NZ, NY, TILE, TILE),
            bf(8, ROWS_A, TILE), bf(8, ROWS_A, TILE), bf(8, ROWS_A, TILE), bf(8, ROWS_A, TILE), bf(8, ROWS_A, TILE),
            bf(7, ROWS_A, TILE), bf(5, ROWS_A, TILE),
            bf(7, NY, rb, TILE), bf(5, NY, rb, TILE), bf(NY, rb, TILE), bf(3, rb, TILE), bf(rb, TILE),
            bf(TILE, TILE),
            pltpu.SemaphoreType.DMA((SEMS,)),
            pltpu.SemaphoreType.DMA((SEMS,)),
        ],
        compiler_params=pltpu.CompilerParams(
            collective_id=0, has_side_effects=True, vmem_limit_bytes=58 * 2**20
        ),
    )(
        gate_coords[0, 0].T, gate_count.reshape(-1), down_rows[0].T,
        down_coords[0, 0].T, down_count.reshape(-1),
        tokens, gate_blocks[0, 0], up_blocks[0, 0], down_blocks[0, 0],
    )


def solution(mesh):
    return jax.shard_map(
        body,
        mesh=mesh,
        in_specs=(
            P("gx", "gy"),
            P("gy", "gx", None, None, None),
            P("gy", "gx", None, None, None),
            P("gy", "gx", None, None),
            P("gy", "gx"),
            P("gx", "gy", None, None, None),
            P("gx", None, None),
            P("gx", "gy", None, None),
            P("gx", "gy"),
        ),
        out_specs=P("gx", "gy"),
        check_vma=False,
    )
```

```python
import jax
import jax.numpy as jnp
from jax import lax
from jax.experimental import pallas as pl
from jax.experimental.pallas import tpu as pltpu
from jax.sharding import PartitionSpec as P

MESH = pl.DeviceIdType.MESH
BLOCK = 128
HALF = 64
NX, NY, NZ = 4, 4, 8
DB, FB = 2, 7
CAP, CAPD = 10, 6
TILE = 256
GU = CAP * BLOCK
DOWN_AT = GU
META_AT = GU + CAPD * HALF
PIECE = META_AT + 32
PART = PIECE // 2
WIDE = NY * TILE
HID = FB * HALF
ROWS_A = 160


def place():
    gx, gy = lax.axis_index("gx"), lax.axis_index("gy")
    return lax.div(gy, NY), lax.rem(gy, NY), lax.div(gx, 2), lax.rem(gx, 2)


def dev(x, y, z, c):
    return (2 * z + c, NY * x + y)


def wrap(v, n):
    return lax.rem(v + n, n)


def rcopy(src, dst, send, recv, to):
    return pltpu.make_async_remote_copy(
        src_ref=src, dst_ref=dst, send_sem=send, recv_sem=recv, device_id=to, device_id_type=MESH
    )


def z_of(x, c):
    return lax.rem(2 * x + 3 * c, NZ)


def x_of(z):
    return lax.div(lax.rem(z + 5 * lax.rem(z, 2), NZ), 2)


def hails(x, y, z, c, partner, partner_self):
    barrier = pltpu.get_barrier_semaphore()

    def hail(to):
        pl.semaphore_signal(barrier, inc=1, device_id=to, device_id_type=MESH)

    hail(dev(wrap(x + 1, NX), y, z, c))
    hail(dev(wrap(x - 1, NX), y, z, c))
    hail(dev(x, y, wrap(z + 1, NZ), c))
    hail(dev(x, y, wrap(z - 1, NZ), c))
    for dy in range(1, NY):
        for flip in range(2):
            hail(dev(x, wrap(y + dy, NY), z, c if flip == 0 else 1 - c))
    hail(dev(x, y, z, 1 - c))

    @pl.when(jnp.logical_not(partner_self))
    def _():
        hail(partner)

    return lambda: pl.semaphore_wait(barrier, 11 + jnp.where(partner_self, 0, 1))


def f32(v):
    return v.astype(jnp.float32)


def bf16(v):
    return v.astype(jnp.bfloat16)


E_AT = {0: 0, -1: 1, 1: 2, 2: 3}
ORDER = [4, -2, -3, 3, 2, -1, 1, 0]


def kernel(
    g_coords, g_count, d_rows, d_coords, d_count,
    tok, gate, up, down, out,
    packed, w_all, relayed, xb, dgu, dd, acc, hid, part,
    ay_in1, ay_in2, ay_in3, ay_out, ay_sum, az_in, az_out,
    bz_in, bz_out, b_sum, by_in, by_out, final, send_sem, recv_sem,
):
    x, y, z, c = place()
    t = 1 - 2 * c
    partner = dev(x_of(z), y, z_of(x, c), lax.rem(z, 2))
    partner_self = z == z_of(x, c)
    remote_partner = jnp.logical_not(partner_self)
    wait_all_here = hails(x, y, z, c, partner, partner_self)
    sibling = dev(x, y, z, 1 - c)
    x_up, x_down = dev(wrap(x + t, NX), y, z, c), dev(wrap(x - t, NX), y, z, c)
    y_up, y_down = dev(x, wrap(y + t, NY), z, c), dev(x, wrap(y - t, NY), z, c)
    z_up, z_down = dev(x, y, wrap(z + t, NZ), c), dev(x, y, wrap(z - t, NZ), c)
    sent, events, used = [], [], [0]

    def sem():
        used[0] += 1
        return used[0] - 1

    def go(src, dst, to):
        i = sem()
        copy = rcopy(src, dst, send_sem.at[i], recv_sem.at[i], to)
        copy.start()
        sent.append(copy)
        return copy

    def at(time, fn):
        events.append((time, len(events), fn))

    def run():
        for _, _, fn in sorted(events, key=lambda e: e[:2]):
            fn()
        events.clear()

    def xx(dx):
        return wrap(x + dx * t + NX, NX)

    def yy(dy):
        return wrap(y + dy * t + NY, NY)

    def zz(dz):
        return wrap(z + dz * t + NZ, NZ)

    def xblock(zi, yi, row, rows):
        start = pl.multiple_of(lax.rem(zi, 2) * TILE + row, 32)
        return xb.at[x_of(zi), pl.ds(start, rows), pl.ds(pl.multiple_of(yi * TILE, TILE), TILE)]

    low = lax.broadcasted_iota(jnp.int32, (BLOCK, BLOCK), 1) < HALF
    for s in range(CAP):
        g, u = f32(gate[s]), f32(up[s])
        packed[0, s * BLOCK : (s + 1) * BLOCK, :] = bf16(jnp.where(low, g, pltpu.roll(u, HALF, 1)))
        packed[1, s * BLOCK : (s + 1) * BLOCK, :] = bf16(jnp.where(low, pltpu.roll(g, HALF, 1), u))
    for s in range(CAPD):
        for h in range(2):
            packed[h, DOWN_AT + s * HALF : DOWN_AT + (s + 1) * HALF, :] = down[s, h * HALF : (h + 1) * HALF, :]
    slot_row = lax.broadcasted_iota(jnp.int32, (PIECE - META_AT, BLOCK), 0)
    ids = jnp.full((PIECE - META_AT, BLOCK), 99, jnp.int32)
    for s in range(CAP):
        spot = jnp.where(s < g_count[0], g_coords[0, s] * FB + g_coords[1, s], 99)
        ids = jnp.where(slot_row == s, spot, ids)
    for s in range(CAPD):
        kept = d_rows[d_coords[0, s], NY * x + y]
        spot = jnp.where(s < d_count[0], kept * DB + d_coords[1, s], 99)
        ids = jnp.where(slot_row == CAP + s, spot, ids)
    for h in range(2):
        packed[h, META_AT:PIECE, :] = bf16(f32(ids))

    wait_all_here()

    a_part, b_part = (0, ROWS_A), (ROWS_A, TILE - ROWS_A)

    lands = [sem() for _ in range(NY)]
    relay_at = sem()
    firsts = []

    def half(xi, yi, u):
        start = u * PART if isinstance(u, int) else pl.multiple_of(u * PART, 16)
        return w_all.at[xi, yi, pl.ds(start, PART)]

    def perm_part(rows):
        i = sem()
        src, mine = tok.at[pl.ds(*rows)], xblock(z, y, *rows)
        copy = rcopy(src, xblock(z_of(x, c), y, *rows), send_sem.at[i], recv_sem.at[i], partner)
        here = pltpu.make_async_copy(src, mine, recv_sem.at[i])

        @pl.when(partner_self)
        def _():
            here.start()

        @pl.when(remote_partner)
        def _():
            copy.start()

        return copy, here

    perm_b = perm_part(b_part)
    for h in range(2):
        yd = 2 * c + h
        far = yd == wrap(y + 2, NY)
        for u in range(2):
            i = sem()
            src = packed.at[h, pl.ds(u * PART, PART)]
            same = jnp.logical_and(yd == y, c == u)
            there = rcopy(src, half(x, y, u), send_sem.at[i], recv_sem.at[lands[0] + y], dev(x, yd, z, u))
            hop = rcopy(src, relayed, send_sem.at[i], recv_sem.at[relay_at], dev(x, wrap(y + 1 - 2 * u, NY), z, u))

            @pl.when(far)
            def _(hop=hop):
                hop.start()

            @pl.when(same)
            def _(src=src, u=u):
                pltpu.make_async_copy(src, half(x, y, u), recv_sem.at[lands[0] + y]).start()

            @pl.when(jnp.logical_not(jnp.logical_or(far, same)))
            def _(there=there):
                there.start()

            firsts.append((same, there))
    perm_a = perm_part(a_part)

    def relay():
        pltpu.make_async_copy(relayed, relayed, recv_sem.at[relay_at]).wait()
        i = sem()
        copy = rcopy(relayed, half(x, yy(-1), c), send_sem.at[i], recv_sem.at[lands[0] + yy(-1)], y_up)
        copy.start()
        sent.append(copy)

    at(RELAY_STEP, relay)

    handed = []

    def hand(dx, dy):
        ref = half(xx(dx), yy(dy), c)
        handed.append(go(ref, ref, sibling))
        handed_at[-dx if abs(dx) == 1 else dx, -dy if abs(dy) == 1 else dy] = handed[-1]

    handed_at = {}

    def build(e, dy):
        handed_at[e, dy].wait_recv()
        xa, i = xx(e), yy(dy)

        names = w_all[xa, i, META_AT : META_AT + 16, :]
        names = [jnp.broadcast_to(names[s : s + 1, :], (BLOCK, BLOCK)) for s in range(CAP + CAPD)]

        @pl.loop(0, DB)
        def _(r):
            for h in range(FB):
                w = jnp.zeros((BLOCK, BLOCK), jnp.bfloat16)
                for s in range(CAP):
                    hit = names[s] == (r * FB + h).astype(jnp.bfloat16)
                    w = jnp.where(hit, w_all[xa, i, s * BLOCK : (s + 1) * BLOCK, :], w)
                dgu[xa, pl.ds(pl.multiple_of(i * TILE + r * BLOCK, BLOCK), BLOCK), h * BLOCK : (h + 1) * BLOCK] = w

        for h in range(FB):
            for m in range(DB):
                w = jnp.zeros((HALF, BLOCK), jnp.bfloat16)
                for s in range(CAPD):
                    hit = names[CAP + s][:HALF] == jnp.bfloat16(h * DB + m)
                    at_row = DOWN_AT + s * HALF
                    w = jnp.where(hit, w_all[xa, i, at_row : at_row + HALF, :], w)
                dd[xa, i, h * HALF : (h + 1) * HALF, m * BLOCK : (m + 1) * BLOCK] = w

    for n, dy in enumerate((0, 1, -1, 2)):
        ring = {}

        def first(dy=dy, ring=ring):
            pltpu.make_async_copy(relayed, half(x, yy(dy), c), recv_sem.at[lands[0] + yy(dy)]).wait()
            ring["m1"] = go(half(x, yy(dy), c), half(x, yy(dy), c), x_up)
            ring["o1"] = go(half(x, yy(dy), c), half(x, yy(dy), c), x_down)
            hand(0, dy)

        def second(dy=dy, ring=ring):
            ring["m1"].wait_recv()
            ring["m2"] = go(half(xx(-1), yy(dy), c), half(xx(-1), yy(dy), c), x_up)
            hand(-1, dy)

        def third(dy=dy, ring=ring):
            ring["o1"].wait_recv()
            hand(1, dy)

        def fourth(dy=dy, ring=ring):
            ring["m2"].wait_recv()
            hand(2, dy)

        at(FIRST_AT[dy], first)
        at(SECOND_AT[dy], second)
        at(THIRD_AT[dy], third)
        at(FOURTH_AT[dy], fourth)
    for e in (0, -1, 1, 2):
        for i in (0, 1, -1, 2):
            at(BUILD_AT[e, i], lambda e=e, i=i: build(e, i))

    def pass_on(dz, dy, part_rows, to):
        ref = xblock(zz(dz), yy(dy), *part_rows)
        return go(ref, ref, to)

    def along_y(dz, part_rows, time, then=None):
        ring = {}
        ring["m1"] = pass_on(dz, 0, part_rows, y_up)
        ring["o1"] = pass_on(dz, 0, part_rows, y_down)

        def second():
            ring["m1"].wait_recv()
            ring["m2"] = pass_on(dz, -1, part_rows, y_up)
            if then:
                then(-1)

        def third():
            ring["o1"].wait_recv()
            if then:
                then(1)

        def fourth():
            ring["m2"].wait_recv()
            if then:
                then(2)

        return second, third, fourth

    state = {}

    def z_start(dy):
        state["up", dy] = pass_on(0, dy, b_part, z_up)
        state["down", dy] = pass_on(0, dy, b_part, z_down)

    def z_up_step(k, dy):
        state["up", dy].wait_recv()
        if k < 4:
            state["up", dy] = pass_on(-k, dy, b_part, z_up)

    def z_down_step(k, dy):
        state["down", dy].wait_recv()
        if k < 3:
            state["down", dy] = pass_on(k, dy, b_part, z_down)

    def start_b():
        perm_b[1].wait()
        state["by"] = along_y(0, b_part, 0, z_start)
        z_start(0)

    def start_a():
        perm_a[1].wait()
        state["up"] = pass_on(0, 0, a_part, z_up)
        state["down"] = pass_on(0, 0, a_part, z_down)
        state["ay", 0] = along_y(0, a_part, 0)

    at(START_B, start_b)
    at(START_A, start_a)
    for k in range(1, 5):

        def a_up(k=k):
            state["up"].wait_recv()
            if k < 4:
                state["up"] = pass_on(-k, 0, a_part, z_up)
            state["ay", -k if k < 4 else 4] = along_y(-k, a_part, 0)

        def a_down(k=k):
            state["down"].wait_recv()
            if k < 3:
                state["down"] = pass_on(k, 0, a_part, z_down)
            state["ay", k] = along_y(k, a_part, 0)

        at(AUP_AT[k], a_up)
        if k < 4:
            at(ADOWN_AT[k], a_down)
    for dz in ORDER:
        for j in range(3):
            at((AY0_AT, AY1_AT, AY2_AT)[j][dz], lambda dz=dz, j=j: state["ay", dz][j]())
    for j in range(3):
        at((BY0_AT, BY1_AT, BY2_AT)[j], lambda j=j: state["by"][j]())
    for dy in (0, -1, 1, 2):
        for k in range(1, 5):
            at(ZUP_AT[k, dy], lambda k=k, dy=dy: z_up_step(k, dy))
            if k < 4:
                at(ZDOWN_AT[k, dy], lambda k=k, dy=dy: z_down_step(k, dy))

    def clear():
        acc[...] = jnp.zeros_like(acc)

        @pl.loop(0, NX * NY)
        def _(a):
            dd[lax.div(a, NY), lax.rem(a, NY), HID:, :] = jnp.zeros((2 * TILE - HID, TILE), jnp.bfloat16)

    at(-1, clear)

    def multiply(dz):
        xa = x_of(zz(dz))
        rows = pl.ds(pl.multiple_of(lax.rem(zz(dz), 2) * TILE, TILE), TILE)
        acc[rows, :] += jnp.dot(xb[xa, rows, :], dgu[xa], preferred_element_type=jnp.float32)

    def multiply_if(dz, last):
        here = x_of(zz(dz)) == xx(2)

        @pl.when(here if last else jnp.logical_not(here))
        def _():
            multiply(dz)

    for dz in ORDER:
        if dz in (0, -2, 2):
            at(EARLY_AT[dz], lambda dz=dz: multiply_if(dz, False))
            at(MUL_AT[dz], lambda dz=dz: multiply_if(dz, True))
        else:
            at(MUL_AT[dz], lambda dz=dz: multiply(dz))
    wide = lax.broadcasted_iota(jnp.int32, (TILE, BLOCK), 1) < HALF

    def hide(slice_at):
        rows = pl.ds(pl.multiple_of(slice_at * TILE, TILE), TILE)
        for pair in range(4):
            v = acc[rows, 2 * pair * BLOCK : (2 * pair + 1) * BLOCK]
            one = jax.nn.silu(v) * pltpu.roll(v, HALF, 1)
            if 2 * pair + 1 < FB:
                w = acc[rows, (2 * pair + 1) * BLOCK : (2 * pair + 2) * BLOCK]
                two = jax.nn.silu(pltpu.roll(w, HALF, 1)) * w
            else:
                two = jnp.zeros_like(one)
            hid[rows, pair * BLOCK : (pair + 1) * BLOCK] = bf16(jnp.where(wide, one, two))

    rows_a, rows_b = pl.ds(0, ROWS_A), pl.ds(ROWS_A, TILE - ROWS_A)
    DYS = (2, -1, 1, 0)
    first, direct, second = {}, {}, {}

    def begin(i):
        zi = zz(ORDER[i])
        first[i] = go(part.at[zi, yy(2), rows_a], ay_in1.at[i], y_up)
        direct[i] = go(part.at[zi, yy(-1), rows_a], ay_in3.at[i], y_down)

    def project(i):
        dz = ORDER[i]
        zi = zz(dz)
        mine_rows = hid[pl.ds(pl.multiple_of(lax.rem(zi, 2) * TILE, TILE), TILE), :]
        for dy in DYS:
            part[zi, yy(dy)] = bf16(
                jnp.dot(mine_rows, dd[x_of(zi), yy(dy)], preferred_element_type=jnp.float32)
            )
        for j, dy in enumerate(DYS):
            if dz == 4:
                state["bu", j] = go(part.at[zi, yy(dy), rows_b], bz_in.at[0, j], z_up)
            if dz == -3:
                state["bd", j] = go(part.at[zi, yy(dy), rows_b], bz_in.at[4, j], z_down)

    def a_first(i):
        first[i].wait_recv()
        ay_out[i] = bf16(f32(ay_in1[i]) + f32(part[zz(ORDER[i]), yy(1), rows_a]))
        second[i] = go(ay_out.at[i], ay_in2.at[i], y_up)

    def a_sum(i):
        direct[i].wait_recv()
        second[i].wait_recv()
        ay_sum[i] = bf16(f32(ay_in2[i]) + f32(ay_in3[i]) + f32(part[zz(ORDER[i]), y, rows_a]))
        if ORDER[i] == 4:
            state["au"] = go(ay_sum.at[i], az_in.at[0], z_up)
        if ORDER[i] == -3:
            state["ad"] = go(ay_sum.at[i], az_in.at[4], z_down)

    def chain_a_up(k):
        state["au"].wait_recv()
        if k < 4:
            az_out[k - 1] = bf16(f32(az_in[k - 1]) + f32(ay_sum[ORDER.index(4 - k)]))
            state["au"] = go(az_out.at[k - 1], az_in.at[k], z_up)

    def chain_a_down(k):
        state["ad"].wait_recv()
        if k < 3:
            az_out[k + 2] = bf16(f32(az_in[k + 3]) + f32(ay_sum[ORDER.index(k - 3)]))
            state["ad"] = go(az_out.at[k + 2], az_in.at[k + 4], z_down)

    def chain_b_up(k, j):
        state["bu", j].wait_recv()
        if k < 4:
            bz_out[k - 1, j] = bf16(f32(bz_in[k - 1, j]) + f32(part[zz(4 - k), yy(DYS[j]), rows_b]))
            state["bu", j] = go(bz_out.at[k - 1, j], bz_in.at[k, j], z_up)

    def chain_b_down(k, j):
        state["bd", j].wait_recv()
        if k < 3:
            bz_out[k + 2, j] = bf16(f32(bz_in[k + 3, j]) + f32(part[zz(k - 3), yy(DYS[j]), rows_b]))
            state["bd", j] = go(bz_out.at[k + 2, j], bz_in.at[k + 4, j], z_down)

    def b_end(j):
        b_sum[j] = bf16(f32(bz_in[3, j]) + f32(bz_in[6, j]) + f32(part[z, yy(DYS[j]), rows_b]))
        if j == 0:
            state["by1"] = go(b_sum.at[0], by_in.at[0], y_up)
        if j == 1:
            state["by3"] = go(b_sum.at[1], by_in.at[2], y_down)

    def b_relay():
        state["by1"].wait_recv()
        by_out[...] = bf16(f32(by_in[0]) + f32(b_sum[2]))
        state["by2"] = go(by_out, by_in.at[1], y_up)

    lasts = []

    def deliver(rows):
        i = sem()
        copy = rcopy(final.at[rows], out.at[rows], send_sem.at[i], recv_sem.at[i], partner)
        here = pltpu.make_async_copy(final.at[rows], out.at[rows], recv_sem.at[i])

        @pl.when(partner_self)
        def _():
            here.start()

        @pl.when(remote_partner)
        def _():
            copy.start()

        lasts.append((copy, here))

    def b_last():
        state["by3"].wait_recv()
        state["by2"].wait_recv()
        final[rows_b] = bf16(f32(by_in[1]) + f32(by_in[2]) + f32(b_sum[3]))
        deliver(rows_b)

    def a_last():
        final[rows_a] = bf16(f32(az_in[3]) + f32(az_in[6]) + f32(ay_sum[7]))
        deliver(rows_a)

    even_done = max(MUL_AT[dz] for dz in ORDER if dz % 2 == 0)

    def early():
        hide(lax.rem(z, 2))
        for i in range(2):
            project(i)
            begin(i)

    at(even_done + 0.5, early)
    last_mul = max(MUL_AT.values())
    rs = last_mul + 1
    f, s_at, d = RT["f"], RT["s"], RT["d"]
    at(rs - 0.5, lambda: hide(lax.rem(z + 1, 2)))
    for i in range(8):
        if i >= 2:
            at(rs + 4.2 + 0.45 * (i - 2), lambda i=i: project(i))
            at(rs + max(f + d * (i - 2), 4.2 + 0.45 * (i - 2)) + 0.01, lambda i=i: begin(i))
        at(rs + f + d * i, lambda i=i: a_first(i))
        at(rs + s_at + d * i, lambda i=i: a_sum(i))
    for j in range(4):
        ups = [rs + 5.0 + 0.5 * j] + [rs + b0 + bj * j for b0, bj in RT["up"]]
        downs = [rs + b0 + bj * j for b0, bj in RT["down"]]
        for k in range(1, 5):
            at(ups[k - 1], lambda k=k, j=j: chain_b_up(k, j))
            if k < 4:
                at(downs[k - 1], lambda k=k, j=j: chain_b_down(k, j))
        up = max(ups[3], downs[2])
        at(up + 0.1, lambda j=j: b_end(j))
    at(up + RT["y"], b_relay)
    at(up + 2 * RT["y"], b_last)
    slot = {dz: rs + s_at + d * i + 0.1 for i, dz in enumerate(ORDER)}
    up, down = slot[4], slot[-3]
    for k in range(1, 5):
        up = max(slot[4 - k], up + RT["z"])
        at(up, lambda k=k: chain_a_up(k))
        if k < 4:
            down = max(slot[k - 3], down + RT["z"])
            at(down, lambda k=k: chain_a_down(k))
    at(max(up, down) + 0.1, a_last)
    run()

    for copy in sent:
        copy.wait_send()
    for same, copy in firsts:

        @pl.when(jnp.logical_not(same))
        def _(copy=copy):
            copy.wait_send()

    @pl.when(remote_partner)
    def _():
        perm_a[0].wait_send()
        perm_b[0].wait_send()

    for copy, here in lasts:
        here.wait()

        @pl.when(remote_partner)
        def _(copy=copy):
            copy.wait_send()


SEMS = 200
START_B = 2
START_A = 7
FIRST_AT = {0: 0, 1: 3, -1: 13, 2: 23}
BUILD_AT = {(0, 0): 1, (1, 0): 11, (-1, 0): 12, (0, -1): 14, (0, 1): 18, (0, 2): 28, (1, -1): 40, (2, 0): 42, (-1, 1): 45, (-1, -1): 53, (1, 1): 55, (-1, 2): 59, (1, 2): 62, (2, -1): 76, (2, 1): 78, (2, 2): 81}
RELAY_STEP = 4
ZUP_AT = {(1, 0): 5, (2, 0): 15, (1, 1): 21, (3, 0): 26, (1, -1): 29, (2, 1): 35, (2, -1): 43, (1, 2): 47, (3, 1): 54, (3, -1): 56, (2, 2): 60, (3, 2): 71, (4, 0): 85, (4, -1): 86, (4, 1): 87, (4, 2): 89}
ZDOWN_AT = {(1, 0): 6, (2, 0): 16, (1, 1): 22, (1, -1): 30, (2, 1): 36, (2, -1): 41, (1, 2): 44, (2, 2): 57, (3, 0): 101, (3, 1): 102, (3, -1): 103, (3, 2): 105}
SECOND_AT = {0: 8, 1: 24, -1: 51, 2: 58}
THIRD_AT = {0: 9, 1: 25, -1: 39, 2: 52}
BY1_AT = 10
BY0_AT = 17
AUP_AT = {1: 19, 2: 32, 3: 50, 4: 61}
ADOWN_AT = {1: 20, 2: 33, 3: 48}
AY0_AT = {0: 27, -1: 34, 1: 37, -2: 46, 2: 49, 3: 70, -3: 77, 4: 79}
BY2_AT = 31
FOURTH_AT = {0: 38, 1: 66, -1: 75, 2: 80}
AY1_AT = {0: 63, -2: 67, 2: 72, 4: 88, -1: 92, 1: 95, -3: 98, 3: 104}
AY2_AT = {0: 64, -2: 68, 2: 73, 4: 90, -1: 93, 1: 96, -3: 99, 3: 106}
EARLY_AT = {0: 65, -2: 69, 2: 74}
MUL_AT = {0: 82, -2: 83, 2: 84, 4: 91, -1: 94, 1: 97, -3: 100, 3: 107}
RT = {"f": 3.9, "s": 7.0, "d": 2.7, "y": 2.7, "z": 3.6, "up": ((10.2, 1.0), (15.2, 1.0), (19.6, 0.8)), "down": ((8.4, 1.0), (13.4, 1.0), (18.2, 0.9))}


def body(
    tokens, gate_blocks, up_blocks, gate_coords, gate_count,
    down_blocks, down_rows, down_coords, down_count,
):
    vmem, smem = pl.BlockSpec(memory_space=pltpu.VMEM), pl.BlockSpec(memory_space=pltpu.SMEM)
    rb = TILE - ROWS_A
    bf = lambda *s: pltpu.VMEM(s, jnp.bfloat16)
    return pl.pallas_call(
        kernel,
        out_shape=jax.ShapeDtypeStruct((TILE, TILE), jnp.bfloat16),
        in_specs=[smem] * 5 + [vmem] * 4,
        out_specs=vmem,
        scratch_shapes=[
            bf(2, PIECE, BLOCK), bf(NX, NY, PIECE, BLOCK), bf(PART, BLOCK),
            bf(NX, 2 * TILE, WIDE), bf(NX, WIDE, FB * BLOCK), bf(NX, NY, 2 * TILE, TILE),
            pltpu.VMEM((2 * TILE, FB * BLOCK), jnp.float32), bf(2 * TILE, 2 * TILE),
            bf(NZ, NY, TILE, TILE),
            bf(8, ROWS_A, TILE), bf(8, ROWS_A, TILE), bf(8, ROWS_A, TILE), bf(8, ROWS_A, TILE), bf(8, ROWS_A, TILE),
            bf(7, ROWS_A, TILE), bf(5, ROWS_A, TILE),
            bf(7, NY, rb, TILE), bf(5, NY, rb, TILE), bf(NY, rb, TILE), bf(3, rb, TILE), bf(rb, TILE),
            bf(TILE, TILE),
            pltpu.SemaphoreType.DMA((SEMS,)),
            pltpu.SemaphoreType.DMA((SEMS,)),
        ],
        compiler_params=pltpu.CompilerParams(
            collective_id=0, has_side_effects=True, vmem_limit_bytes=58 * 2**20
        ),
    )(
        gate_coords[0, 0].T, gate_count.reshape(-1), down_rows[0].T,
        down_coords[0, 0].T, down_count.reshape(-1),
        tokens, gate_blocks[0, 0], up_blocks[0, 0], down_blocks[0, 0],
    )


def solution(mesh):
    return jax.shard_map(
        body,
        mesh=mesh,
        in_specs=(
            P("gx", "gy"),
            P("gy", "gx", None, None, None),
            P("gy", "gx", None, None, None),
            P("gy", "gx", None, None),
            P("gy", "gx"),
            P("gx", "gy", None, None, None),
            P("gx", None, None),
            P("gx", "gy", None, None),
            P("gx", "gy"),
        ),
        out_specs=P("gx", "gy"),
        check_vma=False,
    )
```

```python
import jax
import jax.numpy as jnp
from jax import lax
from jax.experimental import pallas as pl
from jax.experimental.pallas import tpu as pltpu
from jax.sharding import PartitionSpec as P

MESH = pl.DeviceIdType.MESH
BLOCK = 128
HALF = 64
NX, NY, NZ = 4, 4, 8
DB, FB = 2, 7
CAP, CAPD = 10, 6
TILE = 256
GU = CAP * BLOCK
DOWN_AT = GU
META_AT = GU + CAPD * HALF
PIECE = META_AT + 32
PART = PIECE // 2
WIDE = NY * TILE
HID = FB * HALF
ROWS_A = 160


def place():
    gx, gy = lax.axis_index("gx"), lax.axis_index("gy")
    return lax.div(gy, NY), lax.rem(gy, NY), lax.div(gx, 2), lax.rem(gx, 2)


def dev(x, y, z, c):
    return (2 * z + c, NY * x + y)


def wrap(v, n):
    return lax.rem(v + n, n)


def rcopy(src, dst, send, recv, to):
    return pltpu.make_async_remote_copy(
        src_ref=src, dst_ref=dst, send_sem=send, recv_sem=recv, device_id=to, device_id_type=MESH
    )


def z_of(x, c):
    return lax.rem(2 * x + 3 * c, NZ)


def x_of(z):
    return lax.div(lax.rem(z + 5 * lax.rem(z, 2), NZ), 2)


def hails(x, y, z, c, partner, partner_self):
    barrier = pltpu.get_barrier_semaphore()

    def hail(to):
        pl.semaphore_signal(barrier, inc=1, device_id=to, device_id_type=MESH)

    hail(dev(wrap(x + 1, NX), y, z, c))
    hail(dev(wrap(x - 1, NX), y, z, c))
    hail(dev(x, y, wrap(z + 1, NZ), c))
    hail(dev(x, y, wrap(z - 1, NZ), c))
    for dy in range(1, NY):
        for flip in range(2):
            hail(dev(x, wrap(y + dy, NY), z, c if flip == 0 else 1 - c))
    hail(dev(x, y, z, 1 - c))

    @pl.when(jnp.logical_not(partner_self))
    def _():
        hail(partner)

    return lambda: pl.semaphore_wait(barrier, 11 + jnp.where(partner_self, 0, 1))


def f32(v):
    return v.astype(jnp.float32)


def bf16(v):
    return v.astype(jnp.bfloat16)


E_AT = {0: 0, -1: 1, 1: 2, 2: 3}
ORDER = [4, -2, -3, 3, 2, -1, 1, 0]


def kernel(
    g_coords, g_count, d_rows, d_coords, d_count,
    tok, gate, up, down, out,
    packed, w_all, relayed, xb, dgu, dd, acc, hid, part,
    ay_in1, ay_in2, ay_in3, ay_out, ay_sum, az_in, az_out,
    bz_in, bz_out, b_sum, by_in, by_out, final, send_sem, recv_sem,
):
    x, y, z, c = place()
    t = 1 - 2 * c
    partner = dev(x_of(z), y, z_of(x, c), lax.rem(z, 2))
    partner_self = z == z_of(x, c)
    remote_partner = jnp.logical_not(partner_self)
    wait_all_here = hails(x, y, z, c, partner, partner_self)
    sibling = dev(x, y, z, 1 - c)
    x_up, x_down = dev(wrap(x + t, NX), y, z, c), dev(wrap(x - t, NX), y, z, c)
    y_up, y_down = dev(x, wrap(y + t, NY), z, c), dev(x, wrap(y - t, NY), z, c)
    z_up, z_down = dev(x, y, wrap(z + t, NZ), c), dev(x, y, wrap(z - t, NZ), c)
    sent, events, used = [], [], [0]

    def sem():
        used[0] += 1
        return used[0] - 1

    def go(src, dst, to):
        i = sem()
        copy = rcopy(src, dst, send_sem.at[i], recv_sem.at[i], to)
        copy.start()
        sent.append(copy)
        return copy

    def at(time, fn):
        events.append((time, len(events), fn))

    def run():
        for _, _, fn in sorted(events, key=lambda e: e[:2]):
            fn()
        events.clear()

    def xx(dx):
        return wrap(x + dx * t + NX, NX)

    def yy(dy):
        return wrap(y + dy * t + NY, NY)

    def zz(dz):
        return wrap(z + dz * t + NZ, NZ)

    def xblock(zi, yi, row, rows):
        start = pl.multiple_of(lax.rem(zi, 2) * TILE + row, 32)
        return xb.at[x_of(zi), pl.ds(start, rows), pl.ds(pl.multiple_of(yi * TILE, TILE), TILE)]

    low = lax.broadcasted_iota(jnp.int32, (BLOCK, BLOCK), 1) < HALF
    for s in range(CAP):
        g, u = f32(gate[s]), f32(up[s])
        packed[0, s * BLOCK : (s + 1) * BLOCK, :] = bf16(jnp.where(low, g, pltpu.roll(u, HALF, 1)))
        packed[1, s * BLOCK : (s + 1) * BLOCK, :] = bf16(jnp.where(low, pltpu.roll(g, HALF, 1), u))
    for s in range(CAPD):
        for h in range(2):
            packed[h, DOWN_AT + s * HALF : DOWN_AT + (s + 1) * HALF, :] = down[s, h * HALF : (h + 1) * HALF, :]
    slot_row = lax.broadcasted_iota(jnp.int32, (PIECE - META_AT, BLOCK), 0)
    ids = jnp.full((PIECE - META_AT, BLOCK), 99, jnp.int32)
    for s in range(CAP):
        spot = jnp.where(s < g_count[0], g_coords[0, s] * FB + g_coords[1, s], 99)
        ids = jnp.where(slot_row == s, spot, ids)
    for s in range(CAPD):
        kept = d_rows[d_coords[0, s], NY * x + y]
        spot = jnp.where(s < d_count[0], kept * DB + d_coords[1, s], 99)
        ids = jnp.where(slot_row == CAP + s, spot, ids)
    for h in range(2):
        packed[h, META_AT:PIECE, :] = bf16(f32(ids))

    wait_all_here()

    a_part, b_part = (0, ROWS_A), (ROWS_A, TILE - ROWS_A)

    lands = [sem() for _ in range(NY)]
    relay_at = sem()
    firsts = []

    def half(xi, yi, u):
        start = u * PART if isinstance(u, int) else pl.multiple_of(u * PART, 16)
        return w_all.at[xi, yi, pl.ds(start, PART)]

    def perm_part(rows):
        i = sem()
        src, mine = tok.at[pl.ds(*rows)], xblock(z, y, *rows)
        copy = rcopy(src, xblock(z_of(x, c), y, *rows), send_sem.at[i], recv_sem.at[i], partner)
        here = pltpu.make_async_copy(src, mine, recv_sem.at[i])

        @pl.when(partner_self)
        def _():
            here.start()

        @pl.when(remote_partner)
        def _():
            copy.start()

        return copy, here

    perm_b = perm_part(b_part)
    for h in range(2):
        yd = 2 * c + h
        far = yd == wrap(y + 2, NY)
        for u in range(2):
            i = sem()
            src = packed.at[h, pl.ds(u * PART, PART)]
            same = jnp.logical_and(yd == y, c == u)
            there = rcopy(src, half(x, y, u), send_sem.at[i], recv_sem.at[lands[0] + y], dev(x, yd, z, u))
            hop = rcopy(src, relayed, send_sem.at[i], recv_sem.at[relay_at], dev(x, wrap(y + 1 - 2 * u, NY), z, u))

            @pl.when(far)
            def _(hop=hop):
                hop.start()

            @pl.when(same)
            def _(src=src, u=u):
                pltpu.make_async_copy(src, half(x, y, u), recv_sem.at[lands[0] + y]).start()

            @pl.when(jnp.logical_not(jnp.logical_or(far, same)))
            def _(there=there):
                there.start()

            firsts.append((same, there))
    perm_a = perm_part(a_part)

    def relay():
        pltpu.make_async_copy(relayed, relayed, recv_sem.at[relay_at]).wait()
        i = sem()
        copy = rcopy(relayed, half(x, yy(-1), c), send_sem.at[i], recv_sem.at[lands[0] + yy(-1)], y_up)
        copy.start()
        sent.append(copy)

    at(RELAY_STEP, relay)

    handed = []

    def hand(dx, dy):
        ref = half(xx(dx), yy(dy), c)
        handed.append(go(ref, ref, sibling))
        handed_at[-dx if abs(dx) == 1 else dx, -dy if abs(dy) == 1 else dy] = handed[-1]

    handed_at = {}

    def build(e, dy):
        handed_at[e, dy].wait_recv()
        xa, i = xx(e), yy(dy)

        names = w_all[xa, i, META_AT : META_AT + 16, :]
        names = [jnp.broadcast_to(names[s : s + 1, :], (BLOCK, BLOCK)) for s in range(CAP + CAPD)]

        @pl.loop(0, DB)
        def _(r):
            for h in range(FB):
                w = jnp.zeros((BLOCK, BLOCK), jnp.bfloat16)
                for s in range(CAP):
                    hit = names[s] == (r * FB + h).astype(jnp.bfloat16)
                    w = jnp.where(hit, w_all[xa, i, s * BLOCK : (s + 1) * BLOCK, :], w)
                dgu[xa, pl.ds(pl.multiple_of(i * TILE + r * BLOCK, BLOCK), BLOCK), h * BLOCK : (h + 1) * BLOCK] = w

        for h in range(FB):
            for m in range(DB):
                w = jnp.zeros((HALF, BLOCK), jnp.bfloat16)
                for s in range(CAPD):
                    hit = names[CAP + s][:HALF] == jnp.bfloat16(h * DB + m)
                    at_row = DOWN_AT + s * HALF
                    w = jnp.where(hit, w_all[xa, i, at_row : at_row + HALF, :], w)
                dd[xa, i, h * HALF : (h + 1) * HALF, m * BLOCK : (m + 1) * BLOCK] = w

    for n, dy in enumerate((0, 1, -1, 2)):
        ring = {}

        def first(dy=dy, ring=ring):
            pltpu.make_async_copy(relayed, half(x, yy(dy), c), recv_sem.at[lands[0] + yy(dy)]).wait()
            ring["m1"] = go(half(x, yy(dy), c), half(x, yy(dy), c), x_up)
            ring["o1"] = go(half(x, yy(dy), c), half(x, yy(dy), c), x_down)
            hand(0, dy)

        def second(dy=dy, ring=ring):
            ring["m1"].wait_recv()
            ring["m2"] = go(half(xx(-1), yy(dy), c), half(xx(-1), yy(dy), c), x_up)
            hand(-1, dy)

        def third(dy=dy, ring=ring):
            ring["o1"].wait_recv()
            hand(1, dy)

        def fourth(dy=dy, ring=ring):
            ring["m2"].wait_recv()
            hand(2, dy)

        at(FIRST_AT[dy], first)
        at(SECOND_AT[dy], second)
        at(THIRD_AT[dy], third)
        at(FOURTH_AT[dy], fourth)
    for e in (0, -1, 1, 2):
        for i in (0, 1, -1, 2):
            at(BUILD_AT[e, i], lambda e=e, i=i: build(e, i))

    def pass_on(dz, dy, part_rows, to):
        ref = xblock(zz(dz), yy(dy), *part_rows)
        return go(ref, ref, to)

    def along_y(dz, part_rows, time, then=None):
        ring = {}
        ring["m1"] = pass_on(dz, 0, part_rows, y_up)
        ring["o1"] = pass_on(dz, 0, part_rows, y_down)

        def second():
            ring["m1"].wait_recv()
            ring["m2"] = pass_on(dz, -1, part_rows, y_up)
            if then:
                then(-1)

        def third():
            ring["o1"].wait_recv()
            if then:
                then(1)

        def fourth():
            ring["m2"].wait_recv()
            if then:
                then(2)

        return second, third, fourth

    state = {}

    def z_start(dy):
        state["up", dy] = pass_on(0, dy, b_part, z_up)
        state["down", dy] = pass_on(0, dy, b_part, z_down)

    def z_up_step(k, dy):
        state["up", dy].wait_recv()
        if k < 4:
            state["up", dy] = pass_on(-k, dy, b_part, z_up)

    def z_down_step(k, dy):
        state["down", dy].wait_recv()
        if k < 3:
            state["down", dy] = pass_on(k, dy, b_part, z_down)

    def start_b():
        perm_b[1].wait()
        state["by"] = along_y(0, b_part, 0, z_start)
        z_start(0)

    def start_a():
        perm_a[1].wait()
        state["up"] = pass_on(0, 0, a_part, z_up)
        state["down"] = pass_on(0, 0, a_part, z_down)
        state["ay", 0] = along_y(0, a_part, 0)

    at(START_B, start_b)
    at(START_A, start_a)
    for k in range(1, 5):

        def a_up(k=k):
            state["up"].wait_recv()
            if k < 4:
                state["up"] = pass_on(-k, 0, a_part, z_up)
            state["ay", -k if k < 4 else 4] = along_y(-k, a_part, 0)

        def a_down(k=k):
            state["down"].wait_recv()
            if k < 3:
                state["down"] = pass_on(k, 0, a_part, z_down)
            state["ay", k] = along_y(k, a_part, 0)

        at(AUP_AT[k], a_up)
        if k < 4:
            at(ADOWN_AT[k], a_down)
    for dz in ORDER:
        for j in range(3):
            at((AY0_AT, AY1_AT, AY2_AT)[j][dz], lambda dz=dz, j=j: state["ay", dz][j]())
    for j in range(3):
        at((BY0_AT, BY1_AT, BY2_AT)[j], lambda j=j: state["by"][j]())
    for dy in (0, -1, 1, 2):
        for k in range(1, 5):
            at(ZUP_AT[k, dy], lambda k=k, dy=dy: z_up_step(k, dy))
            if k < 4:
                at(ZDOWN_AT[k, dy], lambda k=k, dy=dy: z_down_step(k, dy))

    def clear():
        acc[...] = jnp.zeros_like(acc)

        @pl.loop(0, NX * NY)
        def _(a):
            dd[lax.div(a, NY), lax.rem(a, NY), HID:, :] = jnp.zeros((2 * TILE - HID, TILE), jnp.bfloat16)

    at(-1, clear)

    def multiply(dz):
        xa = x_of(zz(dz))
        rows = pl.ds(pl.multiple_of(lax.rem(zz(dz), 2) * TILE, TILE), TILE)
        acc[rows, :] += jnp.dot(xb[xa, rows, :], dgu[xa], preferred_element_type=jnp.float32)

    def multiply_if(dz, last):
        here = x_of(zz(dz)) == xx(2)

        @pl.when(here if last else jnp.logical_not(here))
        def _():
            multiply(dz)

    for dz in ORDER:
        if dz in (0, -2, 2):
            at(EARLY_AT[dz], lambda dz=dz: multiply_if(dz, False))
            at(MUL_AT[dz], lambda dz=dz: multiply_if(dz, True))
        else:
            at(MUL_AT[dz], lambda dz=dz: multiply(dz))
    wide = lax.broadcasted_iota(jnp.int32, (TILE, BLOCK), 1) < HALF

    def hide(slice_at):
        rows = pl.ds(pl.multiple_of(slice_at * TILE, TILE), TILE)
        for pair in range(4):
            v = acc[rows, 2 * pair * BLOCK : (2 * pair + 1) * BLOCK]
            one = jax.nn.silu(v) * pltpu.roll(v, HALF, 1)
            if 2 * pair + 1 < FB:
                w = acc[rows, (2 * pair + 1) * BLOCK : (2 * pair + 2) * BLOCK]
                two = jax.nn.silu(pltpu.roll(w, HALF, 1)) * w
            else:
                two = jnp.zeros_like(one)
            hid[rows, pair * BLOCK : (pair + 1) * BLOCK] = bf16(jnp.where(wide, one, two))

    rows_a, rows_b = pl.ds(0, ROWS_A), pl.ds(ROWS_A, TILE - ROWS_A)
    DYS = (2, -1, 1, 0)
    first, direct, second = {}, {}, {}

    def begin(i):
        zi = zz(ORDER[i])
        first[i] = go(part.at[zi, yy(2), rows_a], ay_in1.at[i], y_up)
        direct[i] = go(part.at[zi, yy(-1), rows_a], ay_in3.at[i], y_down)

    def project(i):
        dz = ORDER[i]
        zi = zz(dz)
        mine_rows = hid[pl.ds(pl.multiple_of(lax.rem(zi, 2) * TILE, TILE), TILE), :]
        for dy in DYS:
            part[zi, yy(dy)] = bf16(
                jnp.dot(mine_rows, dd[x_of(zi), yy(dy)], preferred_element_type=jnp.float32)
            )
        for j, dy in enumerate(DYS):
            if dz == 4:
                state["bu", j] = go(part.at[zi, yy(dy), rows_b], bz_in.at[0, j], z_up)
            if dz == -3:
                state["bd", j] = go(part.at[zi, yy(dy), rows_b], bz_in.at[4, j], z_down)

    def a_first(i):
        first[i].wait_recv()
        ay_out[i] = bf16(f32(ay_in1[i]) + f32(part[zz(ORDER[i]), yy(1), rows_a]))
        second[i] = go(ay_out.at[i], ay_in2.at[i], y_up)

    def a_sum(i):
        direct[i].wait_recv()
        second[i].wait_recv()
        ay_sum[i] = bf16(f32(ay_in2[i]) + f32(ay_in3[i]) + f32(part[zz(ORDER[i]), y, rows_a]))
        if ORDER[i] == 4:
            state["au"] = go(ay_sum.at[i], az_in.at[0], z_up)
        if ORDER[i] == -3:
            state["ad"] = go(ay_sum.at[i], az_in.at[4], z_down)

    def chain_a_up(k):
        state["au"].wait_recv()
        if k < 4:
            az_out[k - 1] = bf16(f32(az_in[k - 1]) + f32(ay_sum[ORDER.index(4 - k)]))
            state["au"] = go(az_out.at[k - 1], az_in.at[k], z_up)

    def chain_a_down(k):
        state["ad"].wait_recv()
        if k < 3:
            az_out[k + 2] = bf16(f32(az_in[k + 3]) + f32(ay_sum[ORDER.index(k - 3)]))
            state["ad"] = go(az_out.at[k + 2], az_in.at[k + 4], z_down)

    def chain_b_up(k, j):
        state["bu", j].wait_recv()
        if k < 4:
            bz_out[k - 1, j] = bf16(f32(bz_in[k - 1, j]) + f32(part[zz(4 - k), yy(DYS[j]), rows_b]))
            state["bu", j] = go(bz_out.at[k - 1, j], bz_in.at[k, j], z_up)

    def chain_b_down(k, j):
        state["bd", j].wait_recv()
        if k < 3:
            bz_out[k + 2, j] = bf16(f32(bz_in[k + 3, j]) + f32(part[zz(k - 3), yy(DYS[j]), rows_b]))
            state["bd", j] = go(bz_out.at[k + 2, j], bz_in.at[k + 4, j], z_down)

    def b_end(j):
        b_sum[j] = bf16(f32(bz_in[3, j]) + f32(bz_in[6, j]) + f32(part[z, yy(DYS[j]), rows_b]))
        if j == 0:
            state["by1"] = go(b_sum.at[0], by_in.at[0], y_up)
        if j == 1:
            state["by3"] = go(b_sum.at[1], by_in.at[2], y_down)

    def b_relay():
        state["by1"].wait_recv()
        by_out[...] = bf16(f32(by_in[0]) + f32(b_sum[2]))
        state["by2"] = go(by_out, by_in.at[1], y_up)

    lasts = []

    def deliver(rows):
        i = sem()
        copy = rcopy(final.at[rows], out.at[rows], send_sem.at[i], recv_sem.at[i], partner)
        here = pltpu.make_async_copy(final.at[rows], out.at[rows], recv_sem.at[i])

        @pl.when(partner_self)
        def _():
            here.start()

        @pl.when(remote_partner)
        def _():
            copy.start()

        lasts.append((copy, here))

    def b_last():
        state["by3"].wait_recv()
        state["by2"].wait_recv()
        final[rows_b] = bf16(f32(by_in[1]) + f32(by_in[2]) + f32(b_sum[3]))
        deliver(rows_b)

    def a_last():
        final[rows_a] = bf16(f32(az_in[3]) + f32(az_in[6]) + f32(ay_sum[7]))
        deliver(rows_a)

    even_done = max(MUL_AT[dz] for dz in ORDER if dz % 2 == 0)

    def early():
        hide(lax.rem(z, 2))
        for i in range(2):
            project(i)
            begin(i)

    at(even_done + 0.5, early)
    last_mul = max(MUL_AT.values())
    rs = last_mul + 1
    f, s_at, d = RT["f"], RT["s"], RT["d"]
    at(rs - 0.5, lambda: hide(lax.rem(z + 1, 2)))
    for i in range(8):
        if i >= 2:
            at(rs + 4.2 + 0.45 * (i - 2), lambda i=i: project(i))
            at(rs + max(f + d * (i - 2), 4.2 + 0.45 * (i - 2)) + 0.01, lambda i=i: begin(i))
        at(rs + f + d * i, lambda i=i: a_first(i))
        at(rs + s_at + d * i, lambda i=i: a_sum(i))
    for j in range(4):
        ups = [rs + 5.0 + 0.5 * j] + [rs + b0 + bj * j for b0, bj in RT["up"]]
        downs = [rs + b0 + bj * j for b0, bj in RT["down"]]
        for k in range(1, 5):
            at(ups[k - 1], lambda k=k, j=j: chain_b_up(k, j))
            if k < 4:
                at(downs[k - 1], lambda k=k, j=j: chain_b_down(k, j))
        up = max(ups[3], downs[2])
        at(up + 0.1, lambda j=j: b_end(j))
    at(up + 1.7, b_relay)
    at(up + 4.5, b_last)
    slot = {dz: rs + s_at + d * i + 0.1 for i, dz in enumerate(ORDER)}
    up, down = slot[4], slot[-3]
    for k in range(1, 5):
        up = max(slot[4 - k], up + RT["z"])
        at(up, lambda k=k: chain_a_up(k))
        if k < 4:
            down = max(slot[k - 3], down + RT["z"])
            at(down, lambda k=k: chain_a_down(k))
    at(max(up, down) + 0.1, a_last)
    run()

    for copy in sent:
        copy.wait_send()
    for same, copy in firsts:

        @pl.when(jnp.logical_not(same))
        def _(copy=copy):
            copy.wait_send()

    @pl.when(remote_partner)
    def _():
        perm_a[0].wait_send()
        perm_b[0].wait_send()

    for copy, here in lasts:
        here.wait()

        @pl.when(remote_partner)
        def _(copy=copy):
            copy.wait_send()


SEMS = 200
START_B = 2
START_A = 7
FIRST_AT = {0: 0, 1: 3, -1: 13, 2: 23}
BUILD_AT = {(0, 0): 1, (1, 0): 11, (-1, 0): 12, (0, -1): 14, (0, 1): 18, (0, 2): 28, (1, -1): 40, (2, 0): 42, (-1, 1): 45, (-1, -1): 53, (1, 1): 55, (-1, 2): 59, (1, 2): 62, (2, -1): 76, (2, 1): 78, (2, 2): 81}
RELAY_STEP = 4
ZUP_AT = {(1, 0): 5, (2, 0): 15, (1, 1): 21, (3, 0): 26, (1, -1): 29, (2, 1): 35, (2, -1): 43, (1, 2): 47, (3, 1): 54, (3, -1): 56, (2, 2): 60, (3, 2): 71, (4, 0): 85, (4, -1): 86, (4, 1): 87, (4, 2): 89}
ZDOWN_AT = {(1, 0): 6, (2, 0): 16, (1, 1): 22, (1, -1): 30, (2, 1): 36, (2, -1): 41, (1, 2): 44, (2, 2): 57, (3, 0): 101, (3, 1): 102, (3, -1): 103, (3, 2): 105}
SECOND_AT = {0: 8, 1: 24, -1: 51, 2: 58}
THIRD_AT = {0: 9, 1: 25, -1: 39, 2: 52}
BY1_AT = 10
BY0_AT = 17
AUP_AT = {1: 19, 2: 32, 3: 50, 4: 61}
ADOWN_AT = {1: 20, 2: 33, 3: 48}
AY0_AT = {0: 27, -1: 34, 1: 37, -2: 46, 2: 49, 3: 70, -3: 77, 4: 79}
BY2_AT = 31
FOURTH_AT = {0: 38, 1: 66, -1: 75, 2: 80}
AY1_AT = {0: 63, -2: 67, 2: 72, 4: 88, -1: 92, 1: 95, -3: 98, 3: 104}
AY2_AT = {0: 64, -2: 68, 2: 73, 4: 90, -1: 93, 1: 96, -3: 99, 3: 106}
EARLY_AT = {0: 65, -2: 69, 2: 74}
MUL_AT = {0: 82, -2: 83, 2: 84, 4: 91, -1: 94, 1: 97, -3: 100, 3: 107}
RT = {"f": 3.9, "s": 7.0, "d": 2.7, "y": 2.7, "z": 3.6, "up": ((10.2, 1.0), (15.2, 1.0), (19.6, 0.8)), "down": ((8.4, 1.0), (13.4, 1.0), (18.2, 0.9))}


def body(
    tokens, gate_blocks, up_blocks, gate_coords, gate_count,
    down_blocks, down_rows, down_coords, down_count,
):
    vmem, smem = pl.BlockSpec(memory_space=pltpu.VMEM), pl.BlockSpec(memory_space=pltpu.SMEM)
    rb = TILE - ROWS_A
    bf = lambda *s: pltpu.VMEM(s, jnp.bfloat16)
    return pl.pallas_call(
        kernel,
        out_shape=jax.ShapeDtypeStruct((TILE, TILE), jnp.bfloat16),
        in_specs=[smem] * 5 + [vmem] * 4,
        out_specs=vmem,
        scratch_shapes=[
            bf(2, PIECE, BLOCK), bf(NX, NY, PIECE, BLOCK), bf(PART, BLOCK),
            bf(NX, 2 * TILE, WIDE), bf(NX, WIDE, FB * BLOCK), bf(NX, NY, 2 * TILE, TILE),
            pltpu.VMEM((2 * TILE, FB * BLOCK), jnp.float32), bf(2 * TILE, 2 * TILE),
            bf(NZ, NY, TILE, TILE),
            bf(8, ROWS_A, TILE), bf(8, ROWS_A, TILE), bf(8, ROWS_A, TILE), bf(8, ROWS_A, TILE), bf(8, ROWS_A, TILE),
            bf(7, ROWS_A, TILE), bf(5, ROWS_A, TILE),
            bf(7, NY, rb, TILE), bf(5, NY, rb, TILE), bf(NY, rb, TILE), bf(3, rb, TILE), bf(rb, TILE),
            bf(TILE, TILE),
            pltpu.SemaphoreType.DMA((SEMS,)),
            pltpu.SemaphoreType.DMA((SEMS,)),
        ],
        compiler_params=pltpu.CompilerParams(
            collective_id=0, has_side_effects=True, vmem_limit_bytes=58 * 2**20
        ),
    )(
        gate_coords[0, 0].T, gate_count.reshape(-1), down_rows[0].T,
        down_coords[0, 0].T, down_count.reshape(-1),
        tokens, gate_blocks[0, 0], up_blocks[0, 0], down_blocks[0, 0],
    )


def solution(mesh):
    return jax.shard_map(
        body,
        mesh=mesh,
        in_specs=(
            P("gx", "gy"),
            P("gy", "gx", None, None, None),
            P("gy", "gx", None, None, None),
            P("gy", "gx", None, None),
            P("gy", "gx"),
            P("gx", "gy", None, None, None),
            P("gx", None, None),
            P("gx", "gy", None, None),
            P("gx", "gy"),
        ),
        out_specs=P("gx", "gy"),
        check_vma=False,
    )
```
